32 devices in a mesh: mem: 4 (over z), lat: 8 (over y, x, core).
Axes of the slice: x: 2, y: 2, z: 4, core: 2. Of those that a mesh axis runs over, the one named last changes fastest.
Arguments:
- ensemble: bfloat16 [32, 72, 8, 1440], P('mem', None, 'lat'), may hold values from -6 to 6
- truth: bfloat16 [72, 8, 1440], P(None, 'lat'), may hold values from -6 to 6
- row_weight: float32 [8], P('lat'), may hold values from 0.3 to 7, as said below
Outputs:
- loss: float32 [], replicated
- gradient: bfloat16 [32, 72, 8, 1440], P('mem', None, 'lat')
The draws below stay inside these ranges and needn't reach their ends.
Inputs may be any that keep to these rules, and one draw needn't show every extreme that they name: `row_weight`: positive.
All inputs are finite; a program needn't handle non-finite values.
Results may differ from the reference program's by a relative error of at most 0.003.
Values may be sent and summed in bfloat16 or wider, within the bound.
No kernel may reach another device: no remote copies, remote signals or barrier semaphores. Data moves between devices by JAX's collectives and lax.ppermute only.
A program may use at most 128 MiB of HBM per device.

```python
import jax
import jax.numpy as jnp
from jax import lax

C = 72
LON = 1440
M = 32
NLAT = 8


def draw_row_weight(key, part):
    rows = jnp.arange(NLAT).astype(jnp.float32)
    rising = 1.0 + 3.0 * rows / NLAT
    noise = jnp.exp(jax.random.uniform(key, (NLAT,), jnp.float32, jnp.log(0.6), jnp.log(1.6)))
    return (rising * noise).astype(jnp.float32)


def level_of(key, extent, pieces, least, high):
    def one(axis_at, blocks):
        heights = jax.random.uniform(jax.random.fold_in(jax.random.fold_in(key, 6), axis_at), (blocks,), jnp.float32, least / len(pieces), high / len(pieces))
        return jnp.repeat(jnp.exp(heights), extent[axis_at] // blocks).reshape((-1,) + (1,) * (len(extent) - axis_at - 1))

    gain = one(*pieces[0])
    for cut in pieces[1:]:
        gain = gain * one(*cut)
    return gain


def centred(rng, shape, scale, most, shards=(), held_as=jnp.bfloat16):
    array = jax.random.normal(rng, shape, jnp.float32) * scale
    if len(shards) > 0:
        array = level_of(rng, shape, shards, -0.22, 0.18) * array
    return jnp.clip(array, min=-most, max=most).astype(held_as)


def setup_inputs(seed: int = 0) -> dict:
    key_list = jax.random.split(jax.random.key(seed), 4)
    return {
        "ensemble": centred(key_list[0], (M, C, NLAT, LON), 1.0, 6.0, ((0, 4), (2, 8))),
        "truth": centred(key_list[1], (C, NLAT, LON), 1.0, 6.0, ((1, 8),)),
        "row_weight": draw_row_weight(jax.random.fold_in(key_list[3], 71), 0),
    }


def reference(ensemble, truth, row_weight):
    members = ensemble.shape[0]
    channels = ensemble.shape[1]
    by_channel = jnp.moveaxis(ensemble, 1, 0)
    weight = row_weight.astype(jnp.float32)[:, None]

    def channel(pair):
        values = pair[0].astype(jnp.float32)
        target = pair[1].astype(jnp.float32)

        def visit(index, carry):
            spread, count = carry
            other = lax.dynamic_index_in_dim(values, index, 0, keepdims=False)
            diff = values - other
            return spread + jnp.abs(diff), count + jnp.sign(diff)

        zeros = jnp.zeros(values.shape, jnp.float32)
        spread, count = lax.fori_loop(0, members, visit, (zeros, zeros))
        skill = values - target
        cell = jnp.sum(jnp.abs(skill), axis=0) / members - jnp.sum(spread, axis=0) / (2.0 * members * (members - 1))
        partial_value = jnp.sum(weight * cell)
        grad = (weight[None] * (jnp.sign(skill) - count / (members - 1))).astype(jnp.bfloat16)
        return partial_value, grad

    partials, grads = lax.map(channel, (by_channel, truth))
    loss = jnp.sum(partials) / (channels * ensemble.shape[2] * ensemble.shape[3])
    return loss, jnp.moveaxis(grads, 0, 1)
```

```python
import functools

import jax
import jax.numpy as jnp
from jax import lax
from jax.experimental import pallas as pl
from jax.experimental.pallas import tpu as pltpu
from jax.sharding import PartitionSpec as P

LANES = 128
ROWS = 16
TILE = 8


def cdiv(a, b):
    return -(-a // b)


class Plan:
    def __init__(self, channels, cells, groups):
        self.channels, self.cells, self.groups = channels, cells, groups
        self.bands = channels // (ROWS * groups)
        self.cols = cells // LANES
        self.body_rows = self.bands * ROWS * groups
        self.tail = cells - self.cols * LANES
        self.left_tiles = (channels - self.body_rows) // TILE
        self.body = self.bands * self.cols
        self.row_tiles = channels // TILE
        self.per_tile = LANES // self.tail if self.tail else 1
        self.tail_tiles = cdiv(self.row_tiles, self.per_tile) if self.tail else 0
        tiles = self.left_tiles * self.cols + self.tail_tiles
        self.extra = cdiv(tiles, 2 * groups)
        self.tiles = tiles
        self.blocks = self.body + self.extra
        assert channels % TILE == 0 and (self.tail == 0 or LANES % self.tail == 0)


def partner(me, b, groups):
    return lax.bitwise_xor(me, b)


def pairs_of(b, size):
    return [(i, i ^ b) for i in range(size)]


def body_slices(plan, piece, block):
    band, col = divmod(block, plan.cols)
    row = pl.multiple_of((piece * plan.bands + band) * ROWS, ROWS)
    return pl.ds(row, ROWS), pl.ds(col * LANES, LANES)


def take_body(plan, first, count, ens, truth, outs, t_out, sem):
    me = lax.axis_index("mem")
    copies = []
    for b in range(plan.groups):
        piece = partner(me, b, plan.groups)
        for i in range(count):
            rows, cols = body_slices(plan, piece, first + i)
            copies.append(
                pltpu.make_async_copy(
                    ens.at[:, rows, cols], outs[b].at[:, pl.ds(i * ROWS, ROWS), :], sem.at[len(copies)]
                )
            )
    for i in range(count):
        rows, cols = body_slices(plan, me, first + i)
        copies.append(
            pltpu.make_async_copy(truth.at[rows, cols], t_out.at[pl.ds(i * ROWS, ROWS), :], sem.at[len(copies)])
        )
    for c in copies:
        c.start()
    return copies


def pack_body_kernel(plan, first, count, ens, truth, *refs):
    outs, t_out, sem = refs[: plan.groups], refs[plan.groups], refs[plan.groups + 1]
    for c in take_body(plan, first, count, ens, truth, outs, t_out, sem):
        c.wait()


def gather_extra(plan, edge, low, extra, lead):
    pad = plan.extra * ROWS * plan.groups - plan.tiles * TILE
    if pad:
        extra[lead + (pl.ds(plan.tiles * TILE, pad), slice(None))] = jnp.zeros((pad, LANES), jnp.bfloat16)
    at = 0
    for r in range(plan.left_tiles):
        for c in range(plan.cols):
            extra[lead + (pl.ds(at * TILE, TILE), slice(None))] = low[
                lead + (pl.ds(r * TILE, TILE), pl.ds(c * LANES, LANES))
            ]
            at += 1
    lane = lax.broadcasted_iota(jnp.int32, (TILE, LANES), 1)
    for t in range(plan.tail_tiles):
        value = jnp.zeros((TILE, LANES), jnp.float32)
        for i in range(plan.per_tile):
            r = t * plan.per_tile + i
            if r < plan.row_tiles:
                one = edge[lead + (pl.ds(r * TILE, TILE), slice(None))].astype(jnp.float32)
                if i:
                    one = pltpu.roll(one, i * plan.tail, 1)
                inside = (lane >= i * plan.tail) & (lane < (i + 1) * plan.tail)
                value = jnp.where(inside, one, value)
        extra[lead + (pl.ds(at * TILE, TILE), slice(None))] = value.astype(jnp.bfloat16)
        at += 1


def pack_rest_kernel(plan, first, count, ens, truth, ens_edge, ens_low, t_edge, t_low, *refs):
    n = plan.groups
    outs, t_out, sem, extra, t_extra = refs[:n], refs[n], refs[n + 1], refs[n + 2], refs[n + 3]
    copies = take_body(plan, first, count, ens, truth, outs, t_out, sem)
    me = lax.axis_index("mem")
    rows = plan.extra * ROWS
    members = ens.shape[0]
    for m in range(members):
        gather_extra(plan, ens_edge, ens_low, extra, (m,))
    gather_extra(plan, t_edge, t_low, t_extra, ())
    for b in range(n):
        at = pl.multiple_of(partner(me, b, n) * rows, ROWS)
        for m in range(members):
            outs[b][m, pl.ds(count * ROWS, rows), :] = extra[m, pl.ds(at, rows), :]
    t_out[pl.ds(count * ROWS, rows), :] = t_extra[pl.ds(pl.multiple_of(me * rows, ROWS), rows), :]
    for c in copies:
        c.wait()


VMEM = pl.BlockSpec(memory_space=pltpu.VMEM)
ANY = pl.BlockSpec(memory_space=pl.ANY)


def pack(plan, ens, truth, first, count, with_extra):
    members = ens.shape[0]
    rows = (count + (plan.extra if with_extra else 0)) * ROWS
    n = plan.groups
    shapes = [jax.ShapeDtypeStruct((members, rows, LANES), jnp.bfloat16)] * n
    shapes.append(jax.ShapeDtypeStruct((rows, LANES), jnp.bfloat16))
    sems = pltpu.SemaphoreType.DMA(((n + 1) * count,))
    if not with_extra:
        return pl.pallas_call(
            functools.partial(pack_body_kernel, plan, first, count),
            out_shape=shapes,
            in_specs=[ANY, ANY],
            out_specs=[VMEM] * (n + 1),
            scratch_shapes=[sems],
            name="pack_body",
        )(ens, truth)
    low = (plan.channels - plan.body_rows)
    specs = [
        ANY,
        ANY,
        pl.BlockSpec((members, plan.channels, LANES), lambda i: (0, 0, plan.cols)),
        pl.BlockSpec((members, low, plan.cells), lambda i: (0, plan.body_rows // low, 0)),
        pl.BlockSpec((plan.channels, LANES), lambda i: (0, plan.cols)),
        pl.BlockSpec((low, plan.cells), lambda i: (plan.body_rows // low, 0)),
    ]
    all_rows = plan.extra * ROWS * n
    return pl.pallas_call(
        functools.partial(pack_rest_kernel, plan, first, count),
        grid=(1,),
        out_shape=shapes,
        in_specs=specs,
        out_specs=[pl.BlockSpec(s.shape, lambda i, k=len(s.shape): (0,) * k) for s in shapes],
        scratch_shapes=[
            sems,
            pltpu.VMEM((members, all_rows, LANES), jnp.bfloat16),
            pltpu.VMEM((all_rows, LANES), jnp.bfloat16),
        ],
        name="pack_rest",
    )(ens, truth, ens, ens, truth, truth)


def sign_of(diff):
    big = jnp.asarray(2.0**127, jnp.bfloat16)
    one = jnp.asarray(1.0, jnp.bfloat16)
    return jnp.minimum(jnp.maximum(diff * big, -one), one)


def count_kernel(n, members, blocks, scale, weight, t_ref, *refs):
    vals, before, grads, loss, counts = refs[:n], refs[n], refs[n + 1 : 2 * n + 1], refs[2 * n + 1], refs[2 * n + 2]
    local = members // n
    w = weight[0]
    step = w / (members - 1.0)

    def block(i, total):
        rows = pl.ds(pl.multiple_of(i * ROWS, ROWS), ROWS)

        def load(g):
            return [vals[g][m, rows, :] for m in range(local)]

        for a in range(n):
            ea = load(a)
            ca = [counts[a * local + m] if a else None for m in range(local)]

            def bump(old, s, up):
                if old is None:
                    return s if up else -s
                return old + s if up else old - s

            for k in range(local):
                for j in range(k + 1, local):
                    s = sign_of(ea[k] - ea[j])
                    ca[k] = bump(ca[k], s, True)
                    ca[j] = bump(ca[j], s, False)
            for b in range(a + 1, n):
                eb = load(b)
                for j in range(local):
                    cj = counts[b * local + j] if a else None
                    for k in range(local):
                        s = sign_of(ea[k] - eb[j])
                        ca[k] = bump(ca[k], s, True)
                        cj = bump(cj, s, False)
                    counts[b * local + j] = cj
            t = t_ref[rows, :]
            t32 = t.astype(jnp.float32)
            most = jnp.asarray(members - 1.0, jnp.bfloat16)
            for k in range(local):
                num = (most * sign_of(ea[k] - t) - ca[k]).astype(jnp.float32)
                grads[a][k, rows, :] = (num * step).astype(jnp.bfloat16)
                total = total + (ea[k].astype(jnp.float32) - t32) * num
        return total

    total = lax.fori_loop(0, blocks, block, jnp.zeros((ROWS, LANES), jnp.float32))
    loss[...] = before[...] + jnp.sum(total) * (w * scale)


def count_terms(values, target, weight, before, scale, members):
    n = len(values)
    local, rows, _ = values[0].shape
    blocks = rows // ROWS
    return pl.pallas_call(
        functools.partial(count_kernel, n, members, blocks, scale),
        out_shape=[jax.ShapeDtypeStruct(v.shape, jnp.bfloat16) for v in values]
        + [jax.ShapeDtypeStruct((TILE, LANES), jnp.float32)],
        in_specs=[pl.BlockSpec(memory_space=pltpu.SMEM)] + [VMEM] * (n + 2),
        out_specs=[VMEM] * (n + 1),
        scratch_shapes=[pltpu.VMEM((members, ROWS, LANES), jnp.bfloat16)],
        cost_estimate=pl.CostEstimate(
            flops=members * members * 3 * rows * LANES, bytes_accessed=4 * n * local * rows * LANES, transcendentals=0
        ),
        name="count",
    )(weight, target, *values, before)


def spread_extra(plan, extra, edge, lead):
    at = plan.left_tiles * plan.cols
    for t in range(plan.tail_tiles):
        value = extra[lead + (pl.ds((at + t) * TILE, TILE), slice(None))].astype(jnp.float32)
        for i in range(plan.per_tile):
            r = t * plan.per_tile + i
            if r < plan.row_tiles:
                one = pltpu.roll(value, LANES - i * plan.tail, 1) if i else value
                edge[lead + (pl.ds(r * TILE, TILE), slice(None))] = one.astype(jnp.bfloat16)


def edge_kernel(plan, count, *refs):
    n = plan.groups
    ins, out, extra = refs[:n], refs[n], refs[n + 1]
    me = lax.axis_index("mem")
    rows = plan.extra * ROWS
    members = ins[0].shape[0]
    for b in range(n):
        at = pl.multiple_of(partner(me, b, n) * rows, ROWS)
        for m in range(members):
            extra[m, pl.ds(at, rows), :] = ins[b][m, pl.ds(count * ROWS, rows), :]
    for m in range(members):
        spread_extra(plan, extra, out, (m,))


def write_edge(plan, pieces, count):
    members = pieces[0].shape[0]
    n = plan.groups
    full = lambda s: pl.BlockSpec(s, lambda i, k=len(s): (0,) * k)
    all_rows = plan.extra * ROWS * n
    return pl.pallas_call(
        functools.partial(edge_kernel, plan, count),
        grid=(1,),
        out_shape=jax.ShapeDtypeStruct((members, plan.channels, plan.cells), jnp.bfloat16),
        in_specs=[full(p.shape) for p in pieces],
        out_specs=pl.BlockSpec((members, plan.channels, LANES), lambda i: (0, 0, plan.cols)),
        scratch_shapes=[pltpu.VMEM((members, all_rows, LANES), jnp.bfloat16)],
        name="write_edge",
    )(*pieces)


def put_kernel(plan, first, count, with_extra, which, *refs):
    n = len(which)
    ins, out, sem = refs[1 : n + 1], refs[n + 1], refs[n + 2]
    me = lax.axis_index("mem")
    copies = []
    for p, b in enumerate(which):
        piece = partner(me, b, plan.groups)
        for i in range(count):
            rows, cols = body_slices(plan, piece, first + i)
            copies.append(
                pltpu.make_async_copy(
                    ins[p].at[:, pl.ds(i * ROWS, ROWS), :], out.at[:, rows, cols], sem.at[len(copies)]
                )
            )
    for c in copies:
        c.start()
    if with_extra:
        per = 2 * plan.extra
        total = plan.left_tiles * plan.cols
        for p, b in enumerate(which):
            piece = partner(me, b, plan.groups)
            for i in range(per):
                tile = piece * per + i

                def one(p=p, i=i, tile=tile):
                    row = pl.multiple_of(plan.body_rows + tile // plan.cols * TILE, TILE)
                    col = pl.multiple_of(lax.rem(tile, plan.cols) * LANES, LANES)
                    c = pltpu.make_async_copy(
                        ins[p].at[:, pl.ds(count * ROWS + i * TILE, TILE), :],
                        out.at[:, pl.ds(row, TILE), pl.ds(col, LANES)],
                        sem.at[n * count + p * per + i],
                    )
                    c.start()
                    c.wait()

                pl.when(tile < total)(one)
    for c in copies:
        c.wait()


def put(plan, out, pieces, first, count, with_extra, which):
    n = len(pieces)
    return pl.pallas_call(
        functools.partial(put_kernel, plan, first, count, with_extra, which),
        out_shape=jax.ShapeDtypeStruct(out.shape, out.dtype),
        in_specs=[ANY] + [VMEM] * n,
        out_specs=ANY,
        scratch_shapes=[pltpu.SemaphoreType.DMA((n * (count + 2 * plan.extra),))],
        input_output_aliases={0: 0},
        name="put",
    )(out, *pieces)


def exchange(pieces, groups):
    out = [pieces[0]] + [None] * (groups - 1)
    for b in reversed(range(1, groups)):
        out[b] = lax.ppermute(pieces[b], "mem", pairs_of(b, groups))
    return out


def butterfly(value, axis, size):
    step = 1
    while step < size:
        value = value + lax.ppermute(value, axis, pairs_of(step, size))
        step *= 2
    return value


def on_device(groups, lats, ensemble, truth, row_weight):
    local, channels, rows, cells = ensemble.shape
    members = local * groups
    plan = Plan(channels, cells, groups)
    ens = ensemble.reshape(local, channels, cells)
    tru = truth.reshape(channels, cells)
    scale = 1.0 / (members * (members - 1.0)) / (channels * rows * lats * cells)
    first = plan.body // 2
    rest = plan.body - first

    a = pack(plan, ens, tru, 0, first, False)
    a_in = exchange(a[:groups], groups)
    c = pack(plan, ens, tru, first, rest, True)
    c_in = exchange(c[:groups], groups)

    zero = jnp.zeros((TILE, LANES), jnp.float32)
    *a_grad, part = count_terms(a_in, a[groups], row_weight, zero, scale, members)
    a_out = exchange(a_grad, groups)
    *c_grad, part = count_terms(c_in, c[groups], row_weight, part, scale, members)
    part = butterfly(part, "lat", lats)
    part = butterfly(part, "mem", groups)
    c_out = exchange(c_grad, groups)

    every = tuple(range(groups))
    out = write_edge(plan, c_out, rest)
    out = put(plan, out, a_out, 0, first, False, every)
    out = put(plan, out, c_out, first, rest, True, every)
    return part[0, 0], out.reshape(ensemble.shape)


def solution(mesh):
    placed = (P("mem", None, "lat", None), P(None, "lat", None), P("lat"))
    return jax.shard_map(
        functools.partial(on_device, mesh.shape["mem"], mesh.shape["lat"]),
        mesh=mesh,
        in_specs=placed,
        out_specs=(P(), P("mem", None, "lat", None)),
        check_vma=False,
    )
```

```python
import functools

import jax
import jax.numpy as jnp
from jax import lax
from jax.experimental import pallas as pl
from jax.experimental.pallas import tpu as pltpu
from jax.sharding import PartitionSpec as P


LANES = 128
ROWS = 16
TILE = 8
PARAMS = pltpu.CompilerParams(vmem_limit_bytes=16 * 1024 * 1024)


def cdiv(a, b):
    return -(-a // b)


class Plan:
    def __init__(self, channels, cells, groups):
        self.channels, self.cells, self.groups = channels, cells, groups
        self.bands = channels // (ROWS * groups)
        self.cols = cells // LANES
        self.body_rows = self.bands * ROWS * groups
        self.tail = cells - self.cols * LANES
        self.left_tiles = (channels - self.body_rows) // TILE
        self.body = self.bands * self.cols
        self.row_tiles = channels // TILE
        self.per_tile = LANES // self.tail if self.tail else 1
        self.tail_tiles = cdiv(self.row_tiles, self.per_tile) if self.tail else 0
        tiles = self.left_tiles * self.cols + self.tail_tiles
        self.extra = cdiv(tiles, 2 * groups)
        self.tiles = tiles
        assert channels % TILE == 0 and (self.tail == 0 or LANES % self.tail == 0)


def partner(me, b):
    return lax.bitwise_xor(me, b)


def pairs_of(b, size):
    return [(i, i ^ b) for i in range(size)]


def body_slices(plan, piece, block):
    band, col = divmod(block, plan.cols)
    row = pl.multiple_of((piece * plan.bands + band) * ROWS, ROWS)
    return pl.ds(row, ROWS), pl.ds(col * LANES, LANES)


def take_body(plan, first, count, ens, truth, outs, t_out, sem):
    me = lax.axis_index("mem")
    copies = []
    for b in range(plan.groups):
        piece = partner(me, b)
        for i in range(count):
            rows, cols = body_slices(plan, piece, first + i)
            copies.append(
                pltpu.make_async_copy(
                    ens.at[:, rows, cols], outs[b].at[:, pl.ds(i * ROWS, ROWS), :], sem.at[len(copies)]
                )
            )
    for i in range(count):
        rows, cols = body_slices(plan, me, first + i)
        copies.append(
            pltpu.make_async_copy(truth.at[rows, cols], t_out.at[pl.ds(i * ROWS, ROWS), :], sem.at[len(copies)])
        )
    for c in copies:
        c.start()
    return copies


def pack_body_kernel(plan, first, count, ens, truth, *refs):
    outs, t_out, sem = refs[: plan.groups], refs[plan.groups], refs[plan.groups + 1]
    for c in take_body(plan, first, count, ens, truth, outs, t_out, sem):
        c.wait()


def gather_extra(plan, edge, low, extra, lead):
    pad = plan.extra * ROWS * plan.groups - plan.tiles * TILE
    if pad:
        extra[lead + (pl.ds(plan.tiles * TILE, pad), slice(None))] = jnp.zeros((pad, LANES), jnp.bfloat16)
    at = 0
    for r in range(plan.left_tiles):
        for c in range(plan.cols):
            extra[lead + (pl.ds(at * TILE, TILE), slice(None))] = low[
                lead + (pl.ds(r * TILE, TILE), pl.ds(c * LANES, LANES))
            ]
            at += 1
    lane = lax.broadcasted_iota(jnp.int32, (TILE, LANES), 1)
    for t in range(plan.tail_tiles):
        value = jnp.zeros((TILE, LANES), jnp.float32)
        for i in range(plan.per_tile):
            r = t * plan.per_tile + i
            if r < plan.row_tiles:
                one = edge[lead + (pl.ds(r * TILE, TILE), slice(None))].astype(jnp.float32)
                if i:
                    one = pltpu.roll(one, i * plan.tail, 1)
                inside = (lane >= i * plan.tail) & (lane < (i + 1) * plan.tail)
                value = jnp.where(inside, one, value)
        extra[lead + (pl.ds(at * TILE, TILE), slice(None))] = value.astype(jnp.bfloat16)
        at += 1


def pack_rest_kernel(plan, first, count, ens, truth, ens_edge, ens_low, t_edge, t_low, *refs):
    n = plan.groups
    outs, t_out, sem, extra, t_extra = refs[:n], refs[n], refs[n + 1], refs[n + 2], refs[n + 3]
    copies = take_body(plan, first, count, ens, truth, outs, t_out, sem)
    me = lax.axis_index("mem")
    rows = plan.extra * ROWS
    members = ens.shape[0]
    for m in range(members):
        gather_extra(plan, ens_edge, ens_low, extra, (m,))
    gather_extra(plan, t_edge, t_low, t_extra, ())
    for b in range(n):
        at = pl.multiple_of(partner(me, b) * rows, ROWS)
        for m in range(members):
            outs[b][m, pl.ds(count * ROWS, rows), :] = extra[m, pl.ds(at, rows), :]
    t_out[pl.ds(count * ROWS, rows), :] = t_extra[pl.ds(pl.multiple_of(me * rows, ROWS), rows), :]
    for c in copies:
        c.wait()


VMEM = pl.BlockSpec(memory_space=pltpu.VMEM)
ANY = pl.BlockSpec(memory_space=pl.ANY)


def pack(plan, ens, truth, first, count, with_extra):
    members = ens.shape[0]
    rows = (count + (plan.extra if with_extra else 0)) * ROWS
    n = plan.groups
    shapes = [jax.ShapeDtypeStruct((members, rows, LANES), jnp.bfloat16)] * n
    shapes.append(jax.ShapeDtypeStruct((rows, LANES), jnp.bfloat16))
    sems = pltpu.SemaphoreType.DMA(((n + 1) * count,))
    if not with_extra:
        return pl.pallas_call(
            functools.partial(pack_body_kernel, plan, first, count),
            out_shape=shapes,
            in_specs=[ANY, ANY],
            out_specs=[VMEM] * (n + 1),
            scratch_shapes=[sems],
            compiler_params=PARAMS,
            name="pack_body",
        )(ens, truth)
    low = (plan.channels - plan.body_rows)
    specs = [
        ANY,
        ANY,
        pl.BlockSpec((members, plan.channels, LANES), lambda i: (0, 0, plan.cols)),
        pl.BlockSpec((members, low, plan.cells), lambda i: (0, plan.body_rows // low, 0)),
        pl.BlockSpec((plan.channels, LANES), lambda i: (0, plan.cols)),
        pl.BlockSpec((low, plan.cells), lambda i: (plan.body_rows // low, 0)),
    ]
    all_rows = plan.extra * ROWS * n
    return pl.pallas_call(
        functools.partial(pack_rest_kernel, plan, first, count),
        grid=(1,),
        out_shape=shapes,
        in_specs=specs,
        out_specs=[pl.BlockSpec(s.shape, lambda i, k=len(s.shape): (0,) * k) for s in shapes],
        scratch_shapes=[
            sems,
            pltpu.VMEM((members, all_rows, LANES), jnp.bfloat16),
            pltpu.VMEM((all_rows, LANES), jnp.bfloat16),
        ],
        compiler_params=PARAMS,
        name="pack_rest",
    )(ens, truth, ens, ens, truth, truth)


def sign_of(diff):
    big = jnp.asarray(2.0**127, jnp.bfloat16)
    one = jnp.asarray(1.0, jnp.bfloat16)
    return jnp.minimum(jnp.maximum(diff * big, -one), one)


def count_kernel(n, members, blocks, scale, has_before, weight, t_ref, *refs):
    vals, refs = refs[:n], refs[n:]
    if has_before:
        before, refs = refs[0], refs[1:]
    grads, loss, counts = refs[:n], refs[n], refs[n + 1]
    local = members // n
    w = weight[0]
    step = w / (members - 1.0)

    def block(i, total):
        rows = pl.ds(pl.multiple_of(i * ROWS, ROWS), ROWS)

        def load(g):
            return [vals[g][m, rows, :] for m in range(local)]

        for a in range(n):
            ea = load(a)
            ca = [counts[a * local + m] if a else None for m in range(local)]

            def bump(old, s, up):
                if old is None:
                    return s if up else -s
                return old + s if up else old - s

            for k in range(local):
                for j in range(k + 1, local):
                    s = sign_of(ea[k] - ea[j])
                    ca[k] = bump(ca[k], s, True)
                    ca[j] = bump(ca[j], s, False)
            for b in range(a + 1, n):
                eb = load(b)
                for j in range(local):
                    cj = counts[b * local + j] if a else None
                    for k in range(local):
                        s = sign_of(ea[k] - eb[j])
                        ca[k] = bump(ca[k], s, True)
                        cj = bump(cj, s, False)
                    counts[b * local + j] = cj
            t = t_ref[rows, :]
            t32 = t.astype(jnp.float32)
            most = jnp.asarray(members - 1.0, jnp.bfloat16)
            for k in range(local):
                num = (most * sign_of(ea[k] - t) - ca[k]).astype(jnp.float32)
                grads[a][k, rows, :] = (num * step).astype(jnp.bfloat16)
                total = total + (ea[k].astype(jnp.float32) - t32) * num
        return total

    total = lax.fori_loop(0, blocks, block, jnp.zeros((ROWS, LANES), jnp.float32))
    total = jnp.sum(total) * (w * scale)
    loss[...] = before[...] + total if has_before else jnp.full(loss.shape, total, jnp.float32)


def count_terms(values, target, weight, before, scale, members):
    n = len(values)
    local, rows, _ = values[0].shape
    blocks = rows // ROWS
    return pl.pallas_call(
        functools.partial(count_kernel, n, members, blocks, scale, before is not None),
        out_shape=[jax.ShapeDtypeStruct(v.shape, jnp.bfloat16) for v in values]
        + [jax.ShapeDtypeStruct((TILE, LANES), jnp.float32)],
        in_specs=[pl.BlockSpec(memory_space=pltpu.SMEM)] + [VMEM] * (n + (1 if before is None else 2)),
        out_specs=[VMEM] * (n + 1),
        scratch_shapes=[pltpu.VMEM((members, ROWS, LANES), jnp.bfloat16)],
        cost_estimate=pl.CostEstimate(
            flops=members * members * 3 * rows * LANES, bytes_accessed=4 * n * local * rows * LANES, transcendentals=0
        ),
        compiler_params=PARAMS,
        name="count",
    )(weight, target, *values, *([] if before is None else [before]))


def spread_extra(plan, extra, edge, lead):
    at = plan.left_tiles * plan.cols
    for t in range(plan.tail_tiles):
        value = extra[lead + (pl.ds((at + t) * TILE, TILE), slice(None))].astype(jnp.float32)
        for i in range(plan.per_tile):
            r = t * plan.per_tile + i
            if r < plan.row_tiles:
                one = pltpu.roll(value, LANES - i * plan.tail, 1) if i else value
                edge[lead + (pl.ds(r * TILE, TILE), slice(None))] = one.astype(jnp.bfloat16)


def edge_kernel(plan, count, *refs):
    n = plan.groups
    ins, out, extra = refs[1 : n + 1], refs[n + 1], refs[n + 2]
    me = lax.axis_index("mem")
    rows = plan.extra * ROWS
    members = ins[0].shape[0]
    for b in range(n):
        at = pl.multiple_of(partner(me, b) * rows, ROWS)
        for m in range(members):
            extra[m, pl.ds(at, rows), :] = ins[b][m, pl.ds(count * ROWS, rows), :]
    for m in range(members):
        spread_extra(plan, extra, out, (m,))


def write_edge(plan, out, pieces, count):
    members = pieces[0].shape[0]
    n = plan.groups
    full = lambda s: pl.BlockSpec(s, lambda i, k=len(s): (0,) * k)
    all_rows = plan.extra * ROWS * n
    return pl.pallas_call(
        functools.partial(edge_kernel, plan, count),
        grid=(1,),
        out_shape=jax.ShapeDtypeStruct(out.shape, out.dtype),
        in_specs=[ANY] + [full(p.shape) for p in pieces],
        out_specs=pl.BlockSpec((members, plan.channels, LANES), lambda i: (0, 0, plan.cols)),
        scratch_shapes=[pltpu.VMEM((members, all_rows, LANES), jnp.bfloat16)],
        input_output_aliases={0: 0},
        compiler_params=PARAMS,
        name="write_edge",
    )(out, *pieces)


def put_kernel(plan, first, count, with_extra, skip, *refs):
    n = plan.groups
    ins, out, sem = refs[skip : n + skip], refs[n + skip], refs[n + skip + 1]
    me = lax.axis_index("mem")
    copies = []
    for b in range(n):
        piece = partner(me, b)
        for i in range(count):
            rows, cols = body_slices(plan, piece, first + i)
            copies.append(
                pltpu.make_async_copy(
                    ins[b].at[:, pl.ds(i * ROWS, ROWS), :], out.at[:, rows, cols], sem.at[len(copies)]
                )
            )
    for c in copies:
        c.start()
    late = []
    if with_extra:
        per = 2 * plan.extra
        total = plan.left_tiles * plan.cols
        for b in range(n):
            for i in range(per):
                tile = partner(me, b) * per + i
                row = pl.multiple_of(plan.body_rows + tile // plan.cols * TILE, TILE)
                col = pl.multiple_of(lax.rem(tile, plan.cols) * LANES, LANES)
                copy = pltpu.make_async_copy(
                    ins[b].at[:, pl.ds(count * ROWS + i * TILE, TILE), :],
                    out.at[:, pl.ds(row, TILE), pl.ds(col, LANES)],
                    sem.at[n * count + b * per + i],
                )
                late.append((tile < total, copy))
        for real, copy in late:
            pl.when(real)(copy.start)
    for c in copies:
        c.wait()
    for real, copy in late:
        pl.when(real)(copy.wait)


def put(plan, out, shape, pieces, first, count, with_extra):
    n = plan.groups
    skip = 0 if out is None else 1
    return pl.pallas_call(
        functools.partial(put_kernel, plan, first, count, with_extra, skip),
        out_shape=jax.ShapeDtypeStruct(shape, jnp.bfloat16),
        in_specs=[ANY] * skip + [VMEM] * n,
        out_specs=ANY,
        scratch_shapes=[pltpu.SemaphoreType.DMA((n * (count + 2 * plan.extra),))],
        input_output_aliases={0: 0} if skip else {},
        compiler_params=PARAMS,
        name="put",
    )(*([out] if skip else []), *pieces)


def exchange(pieces, groups, order):
    out = list(pieces)
    for b in order:
        out[b] = lax.ppermute(pieces[b], "mem", pairs_of(b, groups))
    return out


def butterfly(value, axis, size):
    step = 1
    while step < size:
        value = value + lax.ppermute(value, axis, pairs_of(step, size))
        step *= 2
    return value


def sum_over_groups(value, groups):
    got = exchange([value] * groups, groups, range(1, groups))
    me = lax.axis_index("mem")
    total = jnp.zeros_like(value)
    for g in range(groups):
        one = got[0]
        for b in range(1, groups):
            one = jnp.where(lax.bitwise_xor(me, b) == g, got[b], one)
        total = total + one
    return total


def far_first(groups):
    return list(reversed(range(1, groups)))


def on_device(groups, lats, ensemble, truth, row_weight):
    local, channels, rows, cells = ensemble.shape
    members = local * groups
    plan = Plan(channels, cells, groups)
    ens = ensemble.reshape(local, channels, cells)
    tru = truth.reshape(channels, cells)
    scale = 1.0 / (members * (members - 1.0)) / (channels * rows * lats * cells)
    na = max(1, plan.body // 3)
    nc = max(1, plan.body // 5)
    nb = plan.body - na - nc
    far = far_first(groups)

    a = pack(plan, ens, tru, 0, na, False)
    a_in = exchange(a[:groups], groups, far)
    b = pack(plan, ens, tru, na, nb, True)
    b_in = exchange(b[:groups], groups, far)
    c = pack(plan, ens, tru, na + nb, nc, False)
    c_in = exchange(c[:groups], groups, far)

    *a_grad, part = count_terms(a_in, a[groups], row_weight, None, scale, members)
    a_out = exchange(a_grad, groups, far)
    *b_grad, part = count_terms(b_in, b[groups], row_weight, part, scale, members)
    b_out = exchange(b_grad, groups, far)
    *c_grad, part = count_terms(c_in, c[groups], row_weight, part, scale, members)
    part = butterfly(part, "lat", lats)
    total = sum_over_groups(part, groups)
    c_out = exchange(c_grad, groups, far)

    out = put(plan, None, ens.shape, a_out, 0, na, False)
    out = write_edge(plan, out, b_out, nb)
    out = put(plan, out, ens.shape, b_out, na, nb, True)
    out = put(plan, out, ens.shape, c_out, na + nb, nc, False)
    return total[0, 0], out.reshape(ensemble.shape)


def solution(mesh):
    placed = (P("mem", None, "lat", None), P(None, "lat", None), P("lat"))
    groups = mesh.shape["mem"]
    return jax.shard_map(
        functools.partial(on_device, groups, mesh.shape["lat"]),
        mesh=mesh,
        in_specs=placed,
        out_specs=(P(), P("mem", None, "lat", None)),
        check_vma=False,
    )
```

```python
import functools

import jax
import jax.numpy as jnp
from jax import lax
from jax.experimental import pallas as pl
from jax.experimental.pallas import tpu as pltpu
from jax.sharding import PartitionSpec as P


LANES = 128
ROWS = 16
TILE = 8
HALF = 4
PARAMS = pltpu.CompilerParams(vmem_limit_bytes=16 * 1024 * 1024)


def cdiv(a, b):
    return -(-a // b)


class Plan:
    def __init__(self, channels, cells, groups):
        self.channels, self.cells, self.groups = channels, cells, groups
        self.bands = channels // (ROWS * groups)
        self.cols = cells // LANES
        self.body_rows = self.bands * ROWS * groups
        self.tail = cells - self.cols * LANES
        self.left_tiles = (channels - self.body_rows) // TILE
        self.body = self.bands * self.cols
        self.row_tiles = channels // TILE
        self.per_tile = LANES // self.tail
        self.tail_tiles = cdiv(self.row_tiles, self.per_tile)
        self.halves = cdiv(2 * (self.left_tiles * self.cols + self.tail_tiles), groups)
        self.spare = self.halves * HALF
        self.held = cdiv(self.spare, ROWS) * ROWS
        assert channels % TILE == 0 and LANES % self.tail == 0

    def spots(self, tile):
        return [h // self.halves * self.held + h % self.halves * HALF for h in (2 * tile, 2 * tile + 1)]


def partner(me, b):
    return lax.bitwise_xor(me, b)


def pairs_of(b, size):
    return [(i, i ^ b) for i in range(size)]


def body_slices(plan, piece, block):
    band, col = divmod(block, plan.cols)
    row = pl.multiple_of((piece * plan.bands + band) * ROWS, ROWS)
    return pl.ds(row, ROWS), pl.ds(col * LANES, LANES)


def body_of(ref, members, count):
    return ref.at[pl.ds(0, members * count * ROWS), :].reshape(members, count * ROWS, LANES)


def take_body(plan, first, count, ens, outs, sem):
    me = lax.axis_index("mem")
    copies = []
    for b in range(plan.groups):
        piece = partner(me, b)
        out = body_of(outs[b], ens.shape[0], count)
        for i in range(count):
            rows, cols = body_slices(plan, piece, first + i)
            copies.append(
                pltpu.make_async_copy(ens.at[:, rows, cols], out.at[:, pl.ds(i * ROWS, ROWS), :], sem.at[len(copies)])
            )
    for c in copies:
        c.start()
    return copies


def take_truth(plan, truth, outs, chunks, sem):
    me = lax.axis_index("mem")
    copies = []
    for out, (first, count) in zip(outs, chunks):
        for i in range(count):
            rows, cols = body_slices(plan, me, first + i)
            copies.append(
                pltpu.make_async_copy(truth.at[rows, cols], out.at[pl.ds(i * ROWS, ROWS), :], sem.at[len(copies)])
            )
    for c in copies:
        c.start()
    return copies


def pack_body_kernel(plan, first, count, ens, *refs):
    for c in take_body(plan, first, count, ens, refs[: plan.groups], refs[plan.groups]):
        c.wait()


def gather_extra(plan, edge, low, extra, lead):
    def keep(tile, value):
        for i, spot in enumerate(plan.spots(tile)):
            extra[lead + (pl.ds(spot, HALF), slice(None))] = value[i * HALF : (i + 1) * HALF]

    at = 0
    for r in range(plan.left_tiles):
        for c in range(plan.cols):
            keep(at, low[lead + (pl.ds(r * TILE, TILE), pl.ds(c * LANES, LANES))].astype(jnp.float32))
            at += 1
    lane = lax.broadcasted_iota(jnp.int32, (TILE, LANES), 1)
    for t in range(plan.tail_tiles):
        value = jnp.zeros((TILE, LANES), jnp.float32)
        for i in range(plan.per_tile):
            r = t * plan.per_tile + i
            if r < plan.row_tiles:
                one = edge[lead + (pl.ds(r * TILE, TILE), slice(None))].astype(jnp.float32)
                if i:
                    one = pltpu.roll(one, i * plan.tail, 1)
                inside = (lane >= i * plan.tail) & (lane < (i + 1) * plan.tail)
                value = jnp.where(inside, one, value)
        keep(at, value)
        at += 1


def pack_rest_kernel(plan, chunks, at_chunk, ens, truth, ens_edge, ens_low, t_edge, t_low, *refs):
    n, k = plan.groups, len(chunks)
    outs, t_outs = refs[:n], refs[n : n + k]
    sem, t_sem, extra, t_extra = refs[n + k :]
    first, count = chunks[at_chunk]
    copies = take_body(plan, first, count, ens, outs, sem) + take_truth(plan, truth, t_outs, chunks, t_sem)
    me = lax.axis_index("mem")
    members = ens.shape[0]
    body = members * count * ROWS
    extra[...] = jnp.zeros_like(extra)
    t_extra[...] = jnp.zeros_like(t_extra)
    for m in range(members):
        gather_extra(plan, ens_edge, ens_low, extra, (m,))
    gather_extra(plan, t_edge, t_low, t_extra, ())
    for b in range(n):
        at = pl.multiple_of(partner(me, b) * plan.held, ROWS)
        for m in range(members):
            value = extra[m, pl.ds(at, plan.held), :][: plan.spare]
            outs[b][pl.ds(body + m * plan.spare, plan.spare), :] = value.astype(jnp.bfloat16)
    mine = t_extra[pl.ds(pl.multiple_of(me * plan.held, ROWS), plan.held), :]
    t_outs[at_chunk][pl.ds(count * ROWS, plan.held), :] = mine.astype(jnp.bfloat16)
    for c in copies:
        c.wait()


VMEM = pl.BlockSpec(memory_space=pltpu.VMEM)
ANY = pl.BlockSpec(memory_space=pl.ANY)


def flat(members, count, more=0):
    return jax.ShapeDtypeStruct((members * count * ROWS + more, LANES), jnp.bfloat16)


def pack(plan, ens, first, count, params=PARAMS):
    members, n = ens.shape[0], plan.groups
    return pl.pallas_call(
        functools.partial(pack_body_kernel, plan, first, count),
        out_shape=[flat(members, count)] * n,
        in_specs=[ANY],
        out_specs=[VMEM] * n,
        scratch_shapes=[pltpu.SemaphoreType.DMA((n * count,))],
        compiler_params=params,
        name="pack_body",
    )(ens)


def pack_rest(plan, ens, truth, chunks, at_chunk):
    members, n = ens.shape[0], plan.groups
    count = chunks[at_chunk][1]
    shapes = [flat(members, count, members * plan.spare)] * n
    for k, (_, c) in enumerate(chunks):
        shapes.append(flat(1, c, plan.held if k == at_chunk else 0))
    low = plan.channels - plan.body_rows
    specs = [
        ANY,
        ANY,
        pl.BlockSpec((members, plan.channels, LANES), lambda i: (0, 0, plan.cols)),
        pl.BlockSpec((members, low, plan.cells), lambda i: (0, plan.body_rows // low, 0)),
        pl.BlockSpec((plan.channels, LANES), lambda i: (0, plan.cols)),
        pl.BlockSpec((low, plan.cells), lambda i: (plan.body_rows // low, 0)),
    ]
    return pl.pallas_call(
        functools.partial(pack_rest_kernel, plan, chunks, at_chunk),
        grid=(1,),
        out_shape=shapes,
        in_specs=specs,
        out_specs=[pl.BlockSpec(s.shape, lambda i, k=len(s.shape): (0,) * k) for s in shapes],
        scratch_shapes=[
            pltpu.SemaphoreType.DMA((n * count,)),
            pltpu.SemaphoreType.DMA((plan.body,)),
            pltpu.VMEM((members, plan.held * n, LANES), jnp.float32),
            pltpu.VMEM((plan.held * n, LANES), jnp.float32),
        ],
        compiler_params=PARAMS,
        name="pack_rest",
    )(ens, truth, ens, ens, truth, truth)


def sign_of(diff):
    big = jnp.asarray(2.0**127, jnp.bfloat16)
    one = jnp.asarray(1.0, jnp.bfloat16)
    return jnp.minimum(jnp.maximum(diff * big, -one), one)


def count_block(n, local, counts, step, load, t, store, total):
    members = n * local

    def bump(old, s, up):
        if old is None:
            return s if up else -s
        return old + s if up else old - s

    t32 = t.astype(jnp.float32)
    most = jnp.asarray(members - 1.0, jnp.bfloat16)
    for a in range(n):
        ea = [load(a, m) for m in range(local)]
        ca = [counts[a * local + m] if a else None for m in range(local)]
        for k in range(local):
            for j in range(k + 1, local):
                s = sign_of(ea[k] - ea[j])
                ca[k] = bump(ca[k], s, True)
                ca[j] = bump(ca[j], s, False)
        for b in range(a + 1, n):
            eb = [load(b, m) for m in range(local)]
            for j in range(local):
                cj = counts[b * local + j] if a else None
                for k in range(local):
                    s = sign_of(ea[k] - eb[j])
                    ca[k] = bump(ca[k], s, True)
                    cj = bump(cj, s, False)
                counts[b * local + j] = cj
        for k in range(local):
            num = (most * sign_of(ea[k] - t) - ca[k]).astype(jnp.float32)
            store(a, k, (num * step).astype(jnp.bfloat16))
            total = total + (ea[k].astype(jnp.float32) - t32) * num
    return total


def count_kernel(plan, count, local, scale, has_before, with_extra, weight, t_ref, *refs):
    n = plan.groups
    members = n * local
    vals, refs = refs[:n], refs[n:]
    if has_before:
        before, refs = refs[0], refs[1:]
    grads, loss, counts = refs[:n], refs[n], refs[n + 1]
    w = weight[0]
    step = w / (members - 1.0)

    def at(m, i):
        return pl.ds(pl.multiple_of((m * count + i) * ROWS, ROWS), ROWS)

    def block(i, total):
        def store(g, m, value):
            grads[g][at(m, i), :] = value

        t = t_ref[pl.ds(pl.multiple_of(i * ROWS, ROWS), ROWS), :]
        return count_block(n, local, counts, step, lambda g, m: vals[g][at(m, i), :], t, store, total)

    total = lax.fori_loop(0, count, block, jnp.zeros((ROWS, LANES), jnp.float32))
    if with_extra:
        held = refs[n + 2]
        body = local * count * ROWS
        pad = plan.held - plan.spare
        for g in range(n):
            for m in range(local):
                held[g * local + m, pl.ds(0, plan.spare), :] = vals[g][pl.ds(body + m * plan.spare, plan.spare), :]
                if pad:
                    held[g * local + m, pl.ds(plan.spare, pad), :] = jnp.zeros((pad, LANES), jnp.bfloat16)

        def last_block(i, total):
            rows = pl.ds(pl.multiple_of(i * ROWS, ROWS), ROWS)

            def store(g, m, value):
                held[g * local + m, rows, :] = value

            t = t_ref[pl.ds(pl.multiple_of((count + i) * ROWS, ROWS), ROWS), :]
            return count_block(n, local, counts, step, lambda g, m: held[g * local + m, rows, :], t, store, total)

        total = lax.fori_loop(0, plan.held // ROWS, last_block, total)
        for g in range(n):
            for m in range(local):
                grads[g][pl.ds(body + m * plan.spare, plan.spare), :] = held[g * local + m, pl.ds(0, plan.spare), :]
    total = jnp.sum(total) * (w * scale)
    loss[...] = before[...] + total if has_before else jnp.full(loss.shape, total, jnp.float32)


def count_terms(plan, count, values, target, weight, before, scale, members, with_extra, last):
    n = len(values)
    local = members // n
    shape = flat(local, count, TILE) if last else values[0]
    scratch = [pltpu.VMEM((members, ROWS, LANES), jnp.bfloat16)]
    if with_extra:
        scratch.append(pltpu.VMEM((members, plan.held, LANES), jnp.bfloat16))
    cells = target.shape[0] * LANES
    return pl.pallas_call(
        functools.partial(count_kernel, plan, count, local, scale, before is not None, with_extra),
        out_shape=[jax.ShapeDtypeStruct(shape.shape, jnp.bfloat16)] * n
        + [jax.ShapeDtypeStruct((TILE, LANES), jnp.float32)],
        in_specs=[pl.BlockSpec(memory_space=pltpu.SMEM)] + [VMEM] * (n + (1 if before is None else 2)),
        out_specs=[VMEM] * (n + 1),
        scratch_shapes=scratch,
        cost_estimate=pl.CostEstimate(
            flops=members * members * 3 * cells, bytes_accessed=4 * members * cells, transcendentals=0
        ),
        compiler_params=PARAMS,
        name="count",
    )(weight, target, *values, *([] if before is None else [before]))


def attach_kernel(n, part, *refs):
    value = part[...]
    high = value.astype(jnp.bfloat16).astype(jnp.float32)
    mid = (value - high).astype(jnp.bfloat16).astype(jnp.float32)
    row = lax.broadcasted_iota(jnp.int32, value.shape, 0)
    terms = jnp.where(row == 0, high, jnp.where(row == 1, mid, value - high - mid))
    block = jnp.where(row < 3, terms, 0.0).astype(jnp.bfloat16)
    for out in refs[n:]:
        out[pl.ds(out.shape[0] - TILE, TILE), :] = block


def attach(pieces, part):
    n = len(pieces)
    return pl.pallas_call(
        functools.partial(attach_kernel, n),
        out_shape=[jax.ShapeDtypeStruct(p.shape, p.dtype) for p in pieces],
        in_specs=[VMEM] * (n + 1),
        out_specs=[VMEM] * n,
        input_output_aliases={i + 1: i for i in range(n)},
        compiler_params=PARAMS,
        name="attach",
    )(part, *pieces)


def spread_extra(plan, extra, edge, low, lead):
    def take(tile):
        return jnp.concatenate([extra[lead + (pl.ds(spot, HALF), slice(None))] for spot in plan.spots(tile)], axis=0)

    at = 0
    for r in range(plan.left_tiles):
        for c in range(plan.cols):
            low[lead + (pl.ds(r * TILE, TILE), pl.ds(c * LANES, LANES))] = take(at).astype(jnp.bfloat16)
            at += 1
    for t in range(plan.tail_tiles):
        value = take(at + t)
        for i in range(plan.per_tile):
            r = t * plan.per_tile + i
            if r < plan.row_tiles:
                one = pltpu.roll(value, LANES - i * plan.tail, 1) if i else value
                edge[lead + (pl.ds(r * TILE, TILE), slice(None))] = one.astype(jnp.bfloat16)


def edge_kernel(plan, count, *refs):
    n = plan.groups
    ins, out, low, extra = refs[1 : n + 1], refs[n + 1], refs[n + 2], refs[n + 3]
    me = lax.axis_index("mem")
    members = out.shape[0]
    body = members * count * ROWS
    for b in range(n):
        at = pl.multiple_of(partner(me, b) * plan.held, ROWS)
        for m in range(members):
            value = ins[b][pl.ds(body + m * plan.spare, plan.spare), :].astype(jnp.float32)
            extra[m, pl.ds(at, plan.spare), :] = value
    for m in range(members):
        spread_extra(plan, extra, out, low, (m,))


def write_edge(plan, out, pieces, count):
    members = out.shape[0]
    n = plan.groups
    full = lambda s: pl.BlockSpec(s, lambda i, k=len(s): (0,) * k)
    low = (members, plan.left_tiles * TILE, plan.cols * LANES)
    return pl.pallas_call(
        functools.partial(edge_kernel, plan, count),
        grid=(1,),
        out_shape=[jax.ShapeDtypeStruct(out.shape, out.dtype), jax.ShapeDtypeStruct(low, out.dtype)],
        in_specs=[ANY] + [full(p.shape) for p in pieces],
        out_specs=[pl.BlockSpec((members, plan.channels, LANES), lambda i: (0, 0, plan.cols)), full(low)],
        scratch_shapes=[pltpu.VMEM((members, plan.held * n, LANES), jnp.float32)],
        input_output_aliases={0: 0},
        compiler_params=PARAMS,
        name="write_edge",
    )(out, *pieces)


def put_kernel(plan, first, count, skip, last, with_low, *refs):
    n = plan.groups
    ins, refs = refs[skip : n + skip], refs[n + skip :]
    if last:
        part, out, loss, sem, held = refs
    elif with_low:
        low, out, sem = refs
    else:
        out, sem = refs
    me = lax.axis_index("mem")
    members = out.shape[0]
    copies = []
    for b in range(n):
        source = body_of(ins[b], members, count)
        for i in range(count):
            rows, cols = body_slices(plan, partner(me, b), first + i)
            copies.append(
                pltpu.make_async_copy(source.at[:, pl.ds(i * ROWS, ROWS), :], out.at[:, rows, cols], sem.at[len(copies)])
            )
    if with_low:
        rows, cols = pl.ds(plan.body_rows, low.shape[1]), pl.ds(0, low.shape[2])
        copies.append(pltpu.make_async_copy(low, out.at[:, rows, cols], sem.at[len(copies)]))
    for c in copies:
        c.start()
    if last:
        parts = [part[0:1, :]]
        for b in range(1, n):
            block = ins[b][pl.ds(members * count * ROWS, TILE), :].astype(jnp.float32)
            parts.append(block[0:1] + block[1:2] + block[2:3])
        while len(parts) > 1:
            parts = [x + y for x, y in zip(parts[::2], parts[1::2])]
        held[...] = parts[0]
        copies.append(pltpu.make_async_copy(held, loss, sem.at[len(copies)]))
        copies[-1].start()
    for c in copies:
        c.wait()


def put(plan, out, shape, pieces, first, count, low=None, part=None):
    n = plan.groups
    skip = 0 if out is None else 1
    last, with_low = part is not None, low is not None
    shapes = [jax.ShapeDtypeStruct(shape, jnp.bfloat16)]
    if last:
        shapes.append(jax.ShapeDtypeStruct((1, LANES), jnp.float32))
    more = ([part] if last else []) + ([low] if with_low else [])
    return pl.pallas_call(
        functools.partial(put_kernel, plan, first, count, skip, last, with_low),
        out_shape=shapes if last else shapes[0],
        in_specs=[ANY] * skip + [VMEM] * (n + len(more)),
        out_specs=[ANY, ANY] if last else ANY,
        scratch_shapes=[pltpu.SemaphoreType.DMA((n * count + len(more),))]
        + ([pltpu.VMEM((1, LANES), jnp.float32)] if last else []),
        input_output_aliases={0: 0} if skip else {},
        compiler_params=PARAMS,
        name="put",
    )(*([out] if skip else []), *pieces, *more)


def exchange(pieces, groups, order):
    out = list(pieces)
    for b in order:
        out[b] = lax.ppermute(pieces[b], "mem", pairs_of(b, groups))
    return out


def butterfly(value, axis, size):
    step = 1
    while step < size:
        value = value + lax.ppermute(value, axis, pairs_of(step, size))
        step *= 2
    return value


def split(total, parts):
    edges = [round(total * sum(parts[:i]) / sum(parts)) for i in range(len(parts) + 1)]
    return [b - a for a, b in zip(edges, edges[1:])]


PARTS = (4, 6, 3)
EXTRA_IN = 1


def orders(groups, count):
    near = [b for b in range(1, groups)]
    first = [groups - 1] + [b for b in range(1, groups - 1)]
    return [first if k == 0 else near for k in range(count)], [near] * count


def on_device(groups, lats, ensemble, truth, row_weight):
    local, channels, rows, cells = ensemble.shape
    members = local * groups
    plan = Plan(channels, cells, groups)
    ens = ensemble.reshape(local, channels, cells)
    tru = truth.reshape(channels, cells)
    scale = 1.0 / (members * (members - 1.0)) / (channels * rows * lats * cells)
    sizes = split(plan.body + plan.held // ROWS, PARTS)
    sizes[EXTRA_IN] -= plan.held // ROWS
    count = len(sizes)
    chunks = [(sum(sizes[:k]), sizes[k]) for k in range(count)]
    ins, outs = orders(groups, count)

    got = []
    for k in range(count):
        if k == EXTRA_IN:
            made = pack_rest(plan, ens, tru, chunks, k)
            pieces, target = made[:groups], made[groups:]
        else:
            pieces = pack(plan, ens, *chunks[k])
        got.append(exchange(pieces, groups, ins[k]))
    part, back = None, []
    for k in range(count):
        last = k == count - 1
        *grad, part = count_terms(
            plan, sizes[k], got[k], target[k], row_weight, part, scale, members, k == EXTRA_IN, last
        )
        if last:
            part = butterfly(part, "lat", lats)
            grad = grad[:1] + list(attach(grad[1:], part))
        back.append(exchange(grad, groups, outs[k]))
    out = None
    for k in range(count):
        low = None
        if k == EXTRA_IN:
            out, low = write_edge(plan, out, back[k], sizes[k])
        out = put(plan, out, ens.shape, back[k], *chunks[k], low, part if k == count - 1 else None)
    out, loss = out
    return loss[0, 0], out.reshape(ensemble.shape)


def solution(mesh):
    placed = (P("mem", None, "lat", None), P(None, "lat", None), P("lat"))
    groups = mesh.shape["mem"]
    return jax.shard_map(
        functools.partial(on_device, groups, mesh.shape["lat"]),
        mesh=mesh,
        in_specs=placed,
        out_specs=(P(), P("mem", None, "lat", None)),
        check_vma=False,
    )
```

```python
import functools

import jax
import jax.numpy as jnp
from jax import lax
from jax.experimental import pallas as pl
from jax.experimental.pallas import tpu as pltpu
from jax.sharding import PartitionSpec as P


LANES = 128
ROWS = 16
TILE = 8
HALF = 4
PARAMS = pltpu.CompilerParams(vmem_limit_bytes=16 * 1024 * 1024)


def cdiv(a, b):
    return -(-a // b)


class Plan:
    def __init__(self, channels, cells, groups):
        self.channels, self.cells, self.groups = channels, cells, groups
        self.bands = channels // (ROWS * groups)
        self.cols = cells // LANES
        self.body_rows = self.bands * ROWS * groups
        self.tail = cells - self.cols * LANES
        self.left_tiles = (channels - self.body_rows) // TILE
        self.body = self.bands * self.cols
        self.row_tiles = channels // TILE
        self.per_tile = LANES // self.tail
        self.tail_tiles = cdiv(self.row_tiles, self.per_tile)
        self.halves = cdiv(2 * (self.left_tiles * self.cols + self.tail_tiles), groups)
        self.spare = self.halves * HALF
        self.held = cdiv(self.spare, ROWS) * ROWS
        assert channels % TILE == 0 and LANES % self.tail == 0

    def spots(self, tile):
        return [h // self.halves * self.held + h % self.halves * HALF for h in (2 * tile, 2 * tile + 1)]


def partner(me, b):
    return lax.bitwise_xor(me, b)


def pairs_of(b, size):
    return [(i, i ^ b) for i in range(size)]


def body_slices(plan, piece, block):
    band, col = divmod(block, plan.cols)
    row = pl.multiple_of((piece * plan.bands + band) * ROWS, ROWS)
    return pl.ds(row, ROWS), pl.ds(col * LANES, LANES)


def body_of(ref, members, count):
    return ref.at[pl.ds(0, members * count * ROWS), :].reshape(members, count * ROWS, LANES)


def take_body(plan, first, count, ens, outs, sem, which=None):
    me = lax.axis_index("mem")
    copies = []
    which = range(plan.groups) if which is None else which
    for o, b in enumerate(which):
        piece = partner(me, b)
        out = body_of(outs[o], ens.shape[0], count)
        for i in range(count):
            rows, cols = body_slices(plan, piece, first + i)
            copies.append(
                pltpu.make_async_copy(ens.at[:, rows, cols], out.at[:, pl.ds(i * ROWS, ROWS), :], sem.at[len(copies)])
            )
    for c in copies:
        c.start()
    return copies


def take_truth(plan, truth, outs, chunks, sem):
    me = lax.axis_index("mem")
    copies = []
    for out, (first, count) in zip(outs, chunks):
        for i in range(count):
            rows, cols = body_slices(plan, me, first + i)
            copies.append(
                pltpu.make_async_copy(truth.at[rows, cols], out.at[pl.ds(i * ROWS, ROWS), :], sem.at[len(copies)])
            )
    for c in copies:
        c.start()
    return copies


def pack_body_kernel(plan, first, count, which, ens, *refs):
    for c in take_body(plan, first, count, ens, refs[:-1], refs[-1], which):
        c.wait()


def gather_extra(plan, edge, low, extra, lead):
    def keep(tile, value):
        for i, spot in enumerate(plan.spots(tile)):
            extra[lead + (pl.ds(spot, HALF), slice(None))] = value[i * HALF : (i + 1) * HALF]

    at = 0
    for r in range(plan.left_tiles):
        for c in range(plan.cols):
            keep(at, low[lead + (pl.ds(r * TILE, TILE), pl.ds(c * LANES, LANES))].astype(jnp.float32))
            at += 1
    lane = lax.broadcasted_iota(jnp.int32, (TILE, LANES), 1)
    for t in range(plan.tail_tiles):
        value = jnp.zeros((TILE, LANES), jnp.float32)
        for i in range(plan.per_tile):
            r = t * plan.per_tile + i
            if r < plan.row_tiles:
                one = edge[lead + (pl.ds(r * TILE, TILE), slice(None))].astype(jnp.float32)
                if i:
                    one = pltpu.roll(one, i * plan.tail, 1)
                inside = (lane >= i * plan.tail) & (lane < (i + 1) * plan.tail)
                value = jnp.where(inside, one, value)
        keep(at, value)
        at += 1


def pack_rest_kernel(plan, chunks, at_chunk, ens, truth, ens_edge, ens_low, t_edge, t_low, *refs):
    n, k = plan.groups, len(chunks)
    outs, t_outs = refs[:n], refs[n : n + k]
    sem, t_sem, extra, t_extra = refs[n + k :]
    first, count = chunks[at_chunk]
    copies = take_body(plan, first, count, ens, outs, sem) + take_truth(plan, truth, t_outs, chunks, t_sem)
    me = lax.axis_index("mem")
    members = ens.shape[0]
    body = members * count * ROWS
    extra[...] = jnp.zeros_like(extra)
    t_extra[...] = jnp.zeros_like(t_extra)
    for m in range(members):
        gather_extra(plan, ens_edge, ens_low, extra, (m,))
    gather_extra(plan, t_edge, t_low, t_extra, ())
    for b in range(n):
        at = pl.multiple_of(partner(me, b) * plan.held, ROWS)
        for m in range(members):
            value = extra[m, pl.ds(at, plan.held), :][: plan.spare]
            outs[b][pl.ds(body + m * plan.spare, plan.spare), :] = value.astype(jnp.bfloat16)
    mine = t_extra[pl.ds(pl.multiple_of(me * plan.held, ROWS), plan.held), :]
    t_outs[at_chunk][pl.ds(count * ROWS, plan.held), :] = mine.astype(jnp.bfloat16)
    for c in copies:
        c.wait()


VMEM = pl.BlockSpec(memory_space=pltpu.VMEM)
ANY = pl.BlockSpec(memory_space=pl.ANY)


def flat(members, count, more=0):
    return jax.ShapeDtypeStruct((members * count * ROWS + more, LANES), jnp.bfloat16)


def pack(plan, ens, first, count, which):
    members, n = ens.shape[0], len(which)
    return pl.pallas_call(
        functools.partial(pack_body_kernel, plan, first, count, which),
        out_shape=[flat(members, count)] * n,
        in_specs=[ANY],
        out_specs=[VMEM] * n,
        scratch_shapes=[pltpu.SemaphoreType.DMA((n * count,))],
        compiler_params=PARAMS,
        name="pack_body",
    )(ens)


def pack_rest(plan, ens, truth, chunks, at_chunk):
    members, n = ens.shape[0], plan.groups
    count = chunks[at_chunk][1]
    shapes = [flat(members, count, members * plan.spare)] * n
    for k, (_, c) in enumerate(chunks):
        shapes.append(flat(1, c, plan.held if k == at_chunk else 0))
    low = plan.channels - plan.body_rows
    specs = [
        ANY,
        ANY,
        pl.BlockSpec((members, plan.channels, LANES), lambda i: (0, 0, plan.cols)),
        pl.BlockSpec((members, low, plan.cells), lambda i: (0, plan.body_rows // low, 0)),
        pl.BlockSpec((plan.channels, LANES), lambda i: (0, plan.cols)),
        pl.BlockSpec((low, plan.cells), lambda i: (plan.body_rows // low, 0)),
    ]
    return pl.pallas_call(
        functools.partial(pack_rest_kernel, plan, chunks, at_chunk),
        grid=(1,),
        out_shape=shapes,
        in_specs=specs,
        out_specs=[pl.BlockSpec(s.shape, lambda i, k=len(s.shape): (0,) * k) for s in shapes],
        scratch_shapes=[
            pltpu.SemaphoreType.DMA((n * count,)),
            pltpu.SemaphoreType.DMA((plan.body,)),
            pltpu.VMEM((members, plan.held * n, LANES), jnp.float32),
            pltpu.VMEM((plan.held * n, LANES), jnp.float32),
        ],
        compiler_params=PARAMS,
        name="pack_rest",
    )(ens, truth, ens, ens, truth, truth)


def sign_of(diff):
    big = jnp.asarray(2.0**127, jnp.bfloat16)
    one = jnp.asarray(1.0, jnp.bfloat16)
    return jnp.minimum(jnp.maximum(diff * big, -one), one)


def count_block(n, local, counts, step, load, t, store, total):
    members = n * local

    def bump(old, s, up):
        if old is None:
            return s if up else -s
        return old + s if up else old - s

    t32 = t.astype(jnp.float32)
    most = jnp.asarray(members - 1.0, jnp.bfloat16)
    for a in range(n):
        ea = [load(a, m) for m in range(local)]
        ca = [counts[a * local + m] if a else None for m in range(local)]
        for k in range(local):
            for j in range(k + 1, local):
                s = sign_of(ea[k] - ea[j])
                ca[k] = bump(ca[k], s, True)
                ca[j] = bump(ca[j], s, False)
        for b in range(a + 1, n):
            eb = [load(b, m) for m in range(local)]
            for j in range(local):
                cj = counts[b * local + j] if a else None
                for k in range(local):
                    s = sign_of(ea[k] - eb[j])
                    ca[k] = bump(ca[k], s, True)
                    cj = bump(cj, s, False)
                counts[b * local + j] = cj
        for k in range(local):
            num = (most * sign_of(ea[k] - t) - ca[k]).astype(jnp.float32)
            store(a, k, (num * step).astype(jnp.bfloat16))
            total = total + (ea[k].astype(jnp.float32) - t32) * num
    return total


def count_kernel(plan, count, local, scale, has_before, with_extra, weight, t_ref, *refs):
    n = plan.groups
    members = n * local
    vals, refs = refs[:n], refs[n:]
    if has_before:
        before, refs = refs[0], refs[1:]
    grads, loss, counts = refs[:n], refs[n], refs[n + 1]
    w = weight[0]
    step = w / (members - 1.0)

    def at(m, i):
        return pl.ds(pl.multiple_of((m * count + i) * ROWS, ROWS), ROWS)

    def block(i, total):
        def store(g, m, value):
            grads[g][at(m, i), :] = value

        t = t_ref[pl.ds(pl.multiple_of(i * ROWS, ROWS), ROWS), :]
        return count_block(n, local, counts, step, lambda g, m: vals[g][at(m, i), :], t, store, total)

    total = lax.fori_loop(0, count, block, jnp.zeros((ROWS, LANES), jnp.float32))
    if with_extra:
        held = refs[n + 2]
        body = local * count * ROWS
        pad = plan.held - plan.spare
        for g in range(n):
            for m in range(local):
                held[g * local + m, pl.ds(0, plan.spare), :] = vals[g][pl.ds(body + m * plan.spare, plan.spare), :]
                if pad:
                    held[g * local + m, pl.ds(plan.spare, pad), :] = jnp.zeros((pad, LANES), jnp.bfloat16)

        def last_block(i, total):
            rows = pl.ds(pl.multiple_of(i * ROWS, ROWS), ROWS)

            def store(g, m, value):
                held[g * local + m, rows, :] = value

            t = t_ref[pl.ds(pl.multiple_of((count + i) * ROWS, ROWS), ROWS), :]
            return count_block(n, local, counts, step, lambda g, m: held[g * local + m, rows, :], t, store, total)

        total = lax.fori_loop(0, plan.held // ROWS, last_block, total)
        for g in range(n):
            for m in range(local):
                grads[g][pl.ds(body + m * plan.spare, plan.spare), :] = held[g * local + m, pl.ds(0, plan.spare), :]
    total = jnp.sum(total) * (w * scale)
    loss[...] = before[...] + total if has_before else jnp.full(loss.shape, total, jnp.float32)


def count_terms(plan, count, values, target, weight, before, scale, members, with_extra, last):
    n = len(values)
    local = members // n
    shape = flat(local, count, TILE) if last else values[0]
    scratch = [pltpu.VMEM((members, ROWS, LANES), jnp.bfloat16)]
    if with_extra:
        scratch.append(pltpu.VMEM((members, plan.held, LANES), jnp.bfloat16))
    cells = target.shape[0] * LANES
    return pl.pallas_call(
        functools.partial(count_kernel, plan, count, local, scale, before is not None, with_extra),
        out_shape=[jax.ShapeDtypeStruct(shape.shape, jnp.bfloat16)] * n
        + [jax.ShapeDtypeStruct((TILE, LANES), jnp.float32)],
        in_specs=[pl.BlockSpec(memory_space=pltpu.SMEM)] + [VMEM] * (n + (1 if before is None else 2)),
        out_specs=[VMEM] * (n + 1),
        scratch_shapes=scratch,
        cost_estimate=pl.CostEstimate(
            flops=members * members * 3 * cells, bytes_accessed=4 * members * cells, transcendentals=0
        ),
        compiler_params=PARAMS,
        name="count",
    )(weight, target, *values, *([] if before is None else [before]))


def attach_kernel(n, part, *refs):
    value = part[...]
    high = value.astype(jnp.bfloat16).astype(jnp.float32)
    mid = (value - high).astype(jnp.bfloat16).astype(jnp.float32)
    row = lax.broadcasted_iota(jnp.int32, value.shape, 0)
    terms = jnp.where(row == 0, high, jnp.where(row == 1, mid, value - high - mid))
    block = jnp.where(row < 3, terms, 0.0).astype(jnp.bfloat16)
    for out in refs[n:]:
        out[pl.ds(out.shape[0] - TILE, TILE), :] = block


def attach(pieces, part):
    n = len(pieces)
    return pl.pallas_call(
        functools.partial(attach_kernel, n),
        out_shape=[jax.ShapeDtypeStruct(p.shape, p.dtype) for p in pieces],
        in_specs=[VMEM] * (n + 1),
        out_specs=[VMEM] * n,
        input_output_aliases={i + 1: i for i in range(n)},
        compiler_params=PARAMS,
        name="attach",
    )(part, *pieces)


def spread_extra(plan, extra, edge, low, lead):
    def take(tile):
        return jnp.concatenate([extra[lead + (pl.ds(spot, HALF), slice(None))] for spot in plan.spots(tile)], axis=0)

    at = 0
    for r in range(plan.left_tiles):
        for c in range(plan.cols):
            low[lead + (pl.ds(r * TILE, TILE), pl.ds(c * LANES, LANES))] = take(at).astype(jnp.bfloat16)
            at += 1
    for t in range(plan.tail_tiles):
        value = take(at + t)
        for i in range(plan.per_tile):
            r = t * plan.per_tile + i
            if r < plan.row_tiles:
                one = pltpu.roll(value, LANES - i * plan.tail, 1) if i else value
                edge[lead + (pl.ds(r * TILE, TILE), slice(None))] = one.astype(jnp.bfloat16)


def edge_kernel(plan, count, *refs):
    n = plan.groups
    ins, out, low, extra = refs[1 : n + 1], refs[n + 1], refs[n + 2], refs[n + 3]
    me = lax.axis_index("mem")
    members = out.shape[0]
    body = members * count * ROWS
    for b in range(n):
        at = pl.multiple_of(partner(me, b) * plan.held, ROWS)
        for m in range(members):
            value = ins[b][pl.ds(body + m * plan.spare, plan.spare), :].astype(jnp.float32)
            extra[m, pl.ds(at, plan.spare), :] = value
    for m in range(members):
        spread_extra(plan, extra, out, low, (m,))


def write_edge(plan, out, pieces, count):
    members = out.shape[0]
    n = plan.groups
    full = lambda s: pl.BlockSpec(s, lambda i, k=len(s): (0,) * k)
    low = (members, plan.left_tiles * TILE, plan.cols * LANES)
    return pl.pallas_call(
        functools.partial(edge_kernel, plan, count),
        grid=(1,),
        out_shape=[jax.ShapeDtypeStruct(out.shape, out.dtype), jax.ShapeDtypeStruct(low, out.dtype)],
        in_specs=[ANY] + [full(p.shape) for p in pieces],
        out_specs=[pl.BlockSpec((members, plan.channels, LANES), lambda i: (0, 0, plan.cols)), full(low)],
        scratch_shapes=[pltpu.VMEM((members, plan.held * n, LANES), jnp.float32)],
        input_output_aliases={0: 0},
        compiler_params=PARAMS,
        name="write_edge",
    )(out, *pieces)


def put_kernel(plan, first, count, skip, last, with_low, *refs):
    n = plan.groups
    ins, refs = refs[skip : n + skip], refs[n + skip :]
    if last:
        part, out, loss, sem, held = refs
    elif with_low:
        low, out, sem = refs
    else:
        out, sem = refs
    me = lax.axis_index("mem")
    members = out.shape[0]
    copies = []
    for b in range(n):
        source = body_of(ins[b], members, count)
        for i in range(count):
            rows, cols = body_slices(plan, partner(me, b), first + i)
            copies.append(
                pltpu.make_async_copy(source.at[:, pl.ds(i * ROWS, ROWS), :], out.at[:, rows, cols], sem.at[len(copies)])
            )
    if with_low:
        rows, cols = pl.ds(plan.body_rows, low.shape[1]), pl.ds(0, low.shape[2])
        copies.append(pltpu.make_async_copy(low, out.at[:, rows, cols], sem.at[len(copies)]))
    for c in copies:
        c.start()
    if last:
        parts = [part[0:1, :]]
        for b in range(1, n):
            block = ins[b][pl.ds(members * count * ROWS, TILE), :].astype(jnp.float32)
            parts.append(block[0:1] + block[1:2] + block[2:3])
        while len(parts) > 1:
            parts = [x + y for x, y in zip(parts[::2], parts[1::2])]
        held[...] = parts[0]
        copies.append(pltpu.make_async_copy(held, loss, sem.at[len(copies)]))
        copies[-1].start()
    for c in copies:
        c.wait()


def put(plan, out, shape, pieces, first, count, low=None, part=None):
    n = plan.groups
    skip = 0 if out is None else 1
    last, with_low = part is not None, low is not None
    shapes = [jax.ShapeDtypeStruct(shape, jnp.bfloat16)]
    if last:
        shapes.append(jax.ShapeDtypeStruct((1, LANES), jnp.float32))
    more = ([part] if last else []) + ([low] if with_low else [])
    return pl.pallas_call(
        functools.partial(put_kernel, plan, first, count, skip, last, with_low),
        out_shape=shapes if last else shapes[0],
        in_specs=[ANY] * skip + [VMEM] * (n + len(more)),
        out_specs=[ANY, ANY] if last else ANY,
        scratch_shapes=[pltpu.SemaphoreType.DMA((n * count + len(more),))]
        + ([pltpu.VMEM((1, LANES), jnp.float32)] if last else []),
        input_output_aliases={0: 0} if skip else {},
        compiler_params=PARAMS,
        name="put",
    )(*([out] if skip else []), *pieces, *more)


def exchange(pieces, groups, order):
    out = list(pieces)
    for b in order:
        out[b] = lax.ppermute(pieces[b], "mem", pairs_of(b, groups))
    return out


def butterfly(value, axis, size):
    step = 1
    while step < size:
        value = value + lax.ppermute(value, axis, pairs_of(step, size))
        step *= 2
    return value


def split(total, parts):
    edges = [round(total * sum(parts[:i]) / sum(parts)) for i in range(len(parts) + 1)]
    return [b - a for a, b in zip(edges, edges[1:])]


PARTS = (3, 6, 4)
EXTRA_IN = 1


def orders(groups, count):
    near = [b for b in range(1, groups)]
    first = [groups - 1] + [b for b in range(1, groups - 1)]
    end = [near[1], near[0]] + near[2:] if groups > 2 else near
    return [first if k == 0 else near for k in range(count)], [near] * (count - 1) + [end]


def on_device(groups, lats, ensemble, truth, row_weight):
    local, channels, rows, cells = ensemble.shape
    members = local * groups
    plan = Plan(channels, cells, groups)
    ens = ensemble.reshape(local, channels, cells)
    tru = truth.reshape(channels, cells)
    scale = 1.0 / (members * (members - 1.0)) / (channels * rows * lats * cells)
    sizes = split(plan.body + plan.held // ROWS, PARTS)
    sizes[EXTRA_IN] -= plan.held // ROWS
    count = len(sizes)
    chunks = [(sum(sizes[:k]), sizes[k]) for k in range(count)]
    ins, outs = orders(groups, count)

    got = []
    for k in range(count):
        if k == EXTRA_IN:
            made = pack_rest(plan, ens, tru, chunks, k)
            pieces, target = made[:groups], made[groups:]
        else:
            every = tuple(range(groups))
            if k == 0:
                source = pltpu.with_memory_space_constraint(ens, pltpu.HBM)
                head = pack(plan, source, *chunks[k], every[-1:])
                pieces = list(pack(plan, ens, *chunks[k], every[:-1])) + list(head)
            else:
                pieces = pack(plan, ens, *chunks[k], every)
        got.append(exchange(pieces, groups, ins[k]))
    part, back = None, []
    for k in range(count):
        last = k == count - 1
        *grad, part = count_terms(
            plan, sizes[k], got[k], target[k], row_weight, part, scale, members, k == EXTRA_IN, last
        )
        if last:
            part = butterfly(part, "lat", lats)
            grad = grad[:1] + list(attach(grad[1:], part))
        back.append(exchange(grad, groups, outs[k]))
    out = None
    for k in range(count):
        low = None
        if k == EXTRA_IN:
            out, low = write_edge(plan, out, back[k], sizes[k])
        out = put(plan, out, ens.shape, back[k], *chunks[k], low, part if k == count - 1 else None)
    out, loss = out
    return loss[0, 0], out.reshape(ensemble.shape)


def solution(mesh):
    placed = (P("mem", None, "lat", None), P(None, "lat", None), P("lat"))
    groups = mesh.shape["mem"]
    return jax.shard_map(
        functools.partial(on_device, groups, mesh.shape["lat"]),
        mesh=mesh,
        in_specs=placed,
        out_specs=(P(), P("mem", None, "lat", None)),
        check_vma=False,
    )
```

```python
import functools

import jax
import jax.numpy as jnp
from jax import lax
from jax.experimental import pallas as pl
from jax.experimental.pallas import tpu as pltpu
from jax.sharding import PartitionSpec as P


LANES = 128
ROWS = 16
TILE = 8
PARAMS = pltpu.CompilerParams(vmem_limit_bytes=16 * 1024 * 1024)


def cdiv(a, b):
    return -(-a // b)


class Plan:
    def __init__(self, channels, cells, groups):
        self.channels, self.cells, self.groups = channels, cells, groups
        self.bands = channels // (ROWS * groups)
        self.cols = cells // LANES
        self.body_rows = self.bands * ROWS * groups
        self.tail = cells - self.cols * LANES
        self.left_tiles = (channels - self.body_rows) // TILE
        self.body = self.bands * self.cols
        self.folds = LANES // self.tail
        self.folded = channels // self.folds
        self.low_rows = self.left_tiles * TILE * self.cols
        self.spare = cdiv(self.low_rows + self.folded, groups)
        self.held = cdiv(self.spare, ROWS) * ROWS
        assert channels % TILE == 0 and LANES % self.tail == 0 and channels % self.folds == 0

    def more(self, members):
        return cdiv(members * self.spare, TILE) * TILE

    def runs(self, start, count):
        found, at = [], start
        while at < start + count:
            piece, spot = divmod(at, self.spare)
            length = min(self.spare - spot, start + count - at)
            found.append((at - start, piece * self.held + spot, length))
            at += length
        return found


def partner(me, b):
    return lax.bitwise_xor(me, b)


def pairs_of(b, size):
    return [(i, i ^ b) for i in range(size)]


def body_slices(plan, piece, block):
    band, col = divmod(block, plan.cols)
    row = pl.multiple_of((piece * plan.bands + band) * ROWS, ROWS)
    return pl.ds(row, ROWS), pl.ds(col * LANES, LANES)


def body_of(ref, members, count):
    return ref.at[pl.ds(0, members * count * ROWS), :].reshape(members, count * ROWS, LANES)


def take_body(plan, first, count, ens, outs, sem, which=None):
    me = lax.axis_index("mem")
    copies = []
    which = range(plan.groups) if which is None else which
    for o, b in enumerate(which):
        piece = partner(me, b)
        out = body_of(outs[o], ens.shape[0], count)
        for i in range(count):
            rows, cols = body_slices(plan, piece, first + i)
            copies.append(
                pltpu.make_async_copy(ens.at[:, rows, cols], out.at[:, pl.ds(i * ROWS, ROWS), :], sem.at[len(copies)])
            )
    for c in copies:
        c.start()
    return copies


def take_truth(plan, truth, outs, chunks, sem):
    me = lax.axis_index("mem")
    copies = []
    for out, (first, count) in zip(outs, chunks):
        for i in range(count):
            rows, cols = body_slices(plan, me, first + i)
            copies.append(
                pltpu.make_async_copy(truth.at[rows, cols], out.at[pl.ds(i * ROWS, ROWS), :], sem.at[len(copies)])
            )
    for c in copies:
        c.start()
    return copies


def pack_body_kernel(plan, first, count, which, ens, *refs):
    for c in take_body(plan, first, count, ens, refs[:-1], refs[-1], which):
        c.wait()


def gather_extra(plan, edge, low, extra, work, lead):
    for r in range(plan.left_tiles):
        for c in range(plan.cols):
            value = low[lead + (pl.ds(r * TILE, TILE), pl.ds(c * LANES, LANES))].astype(jnp.float32)
            for at, spot, length in plan.runs((r * plan.cols + c) * TILE, TILE):
                extra[lead + (pl.ds(spot, length), slice(None))] = value[at : at + length]
    value = edge[lead + (slice(None), slice(None))].astype(jnp.float32)
    lane = lax.broadcasted_iota(jnp.int32, value.shape, 1)
    fold = None
    for i in range(plan.folds):
        one = pltpu.roll(value, i * plan.tail, 1) if i else value
        work[i] = jnp.where((lane >= i * plan.tail) & (lane < (i + 1) * plan.tail), one, 0.0)
        part = work[i, pl.ds(i * plan.folded, plan.folded), :]
        fold = part if fold is None else fold + part
    for at, spot, length in plan.runs(plan.low_rows, plan.folded):
        extra[lead + (pl.ds(spot, length), slice(None))] = fold[at : at + length]


def pack_rest_kernel(plan, chunks, at_chunk, ens, truth, ens_edge, ens_low, t_edge, t_low, *refs):
    n, k = plan.groups, len(chunks)
    outs, t_outs = refs[:n], refs[n : n + k]
    sem, t_sem, extra, t_extra, work, stage = refs[n + k :]
    first, count = chunks[at_chunk]
    copies = take_body(plan, first, count, ens, outs, sem) + take_truth(plan, truth, t_outs, chunks, t_sem)
    me = lax.axis_index("mem")
    members = ens.shape[0]
    body = members * count * ROWS
    extra[...] = jnp.zeros_like(extra)
    t_extra[...] = jnp.zeros_like(t_extra)
    stage[...] = jnp.zeros_like(stage)
    for m in range(members):
        gather_extra(plan, ens_edge, ens_low, extra, work, (m,))
    gather_extra(plan, t_edge, t_low, t_extra, work, ())
    for b in range(n):
        at = pl.multiple_of(partner(me, b) * plan.held, ROWS)
        for m in range(members):
            stage[pl.ds(m * plan.spare, plan.spare), :] = extra[m, pl.ds(at, plan.held), :][: plan.spare]
        outs[b][pl.ds(body, plan.more(members)), :] = stage[...].astype(jnp.bfloat16)
    mine = t_extra[pl.ds(pl.multiple_of(me * plan.held, ROWS), plan.held), :]
    t_outs[at_chunk][pl.ds(count * ROWS, plan.held), :] = mine.astype(jnp.bfloat16)
    for c in copies:
        c.wait()


VMEM = pl.BlockSpec(memory_space=pltpu.VMEM)
ANY = pl.BlockSpec(memory_space=pl.ANY)


def flat(members, count, more=0):
    return jax.ShapeDtypeStruct((members * count * ROWS + more, LANES), jnp.bfloat16)


def pack(plan, ens, first, count, which):
    members, n = ens.shape[0], len(which)
    return pl.pallas_call(
        functools.partial(pack_body_kernel, plan, first, count, which),
        out_shape=[flat(members, count)] * n,
        in_specs=[ANY],
        out_specs=[VMEM] * n,
        scratch_shapes=[pltpu.SemaphoreType.DMA((n * count,))],
        compiler_params=PARAMS,
        name="pack_body",
    )(ens)


def pack_rest(plan, ens, truth, chunks, at_chunk):
    members, n = ens.shape[0], plan.groups
    count = chunks[at_chunk][1]
    shapes = [flat(members, count, plan.more(members))] * n
    for k, (_, c) in enumerate(chunks):
        shapes.append(flat(1, c, plan.held if k == at_chunk else 0))
    low = plan.channels - plan.body_rows
    specs = [
        ANY,
        ANY,
        pl.BlockSpec((members, plan.channels, LANES), lambda i: (0, 0, plan.cols)),
        pl.BlockSpec((members, low, plan.cells), lambda i: (0, plan.body_rows // low, 0)),
        pl.BlockSpec((plan.channels, LANES), lambda i: (0, plan.cols)),
        pl.BlockSpec((low, plan.cells), lambda i: (plan.body_rows // low, 0)),
    ]
    return pl.pallas_call(
        functools.partial(pack_rest_kernel, plan, chunks, at_chunk),
        grid=(1,),
        out_shape=shapes,
        in_specs=specs,
        out_specs=[pl.BlockSpec(s.shape, lambda i, k=len(s.shape): (0,) * k) for s in shapes],
        scratch_shapes=[
            pltpu.SemaphoreType.DMA((n * count,)),
            pltpu.SemaphoreType.DMA((plan.body,)),
            pltpu.VMEM((members, plan.held * n, LANES), jnp.float32),
            pltpu.VMEM((plan.held * n, LANES), jnp.float32),
            pltpu.VMEM((plan.folds, plan.channels, LANES), jnp.float32),
            pltpu.VMEM((plan.more(members), LANES), jnp.float32),
        ],
        compiler_params=PARAMS,
        name="pack_rest",
    )(ens, truth, ens, ens, truth, truth)


def sign_of(diff):
    big = jnp.asarray(2.0**127, jnp.bfloat16)
    one = jnp.asarray(1.0, jnp.bfloat16)
    return jnp.minimum(jnp.maximum(diff * big, -one), one)


def count_block(n, local, counts, step, load, t, store, total):
    members = n * local

    def bump(old, s, up):
        if old is None:
            return s if up else -s
        return old + s if up else old - s

    t32 = t.astype(jnp.float32)
    most = jnp.asarray(members - 1.0, jnp.bfloat16)
    for a in range(n):
        ea = [load(a, m) for m in range(local)]
        ca = [counts[a * local + m] if a else None for m in range(local)]
        for k in range(local):
            for j in range(k + 1, local):
                s = sign_of(ea[k] - ea[j])
                ca[k] = bump(ca[k], s, True)
                ca[j] = bump(ca[j], s, False)
        for b in range(a + 1, n):
            eb = [load(b, m) for m in range(local)]
            for j in range(local):
                cj = counts[b * local + j] if a else None
                for k in range(local):
                    s = sign_of(ea[k] - eb[j])
                    ca[k] = bump(ca[k], s, True)
                    cj = bump(cj, s, False)
                counts[b * local + j] = cj
        for k in range(local):
            num = (most * sign_of(ea[k] - t) - ca[k]).astype(jnp.float32)
            store(a, k, (num * step).astype(jnp.bfloat16))
            total = total + (ea[k].astype(jnp.float32) - t32) * num
    return total


def count_kernel(plan, count, local, scale, has_before, with_extra, weight, t_ref, *refs):
    n = plan.groups
    members = n * local
    vals, refs = refs[:n], refs[n:]
    if has_before:
        before, refs = refs[0], refs[1:]
    grads, loss, counts = refs[:n], refs[n], refs[n + 1]
    w = weight[0]
    step = w / (members - 1.0)

    def at(m, i):
        return pl.ds(pl.multiple_of((m * count + i) * ROWS, ROWS), ROWS)

    def block(i, total):
        def store(g, m, value):
            grads[g][at(m, i), :] = value

        t = t_ref[pl.ds(pl.multiple_of(i * ROWS, ROWS), ROWS), :]
        return count_block(n, local, counts, step, lambda g, m: vals[g][at(m, i), :], t, store, total)

    total = lax.fori_loop(0, count, block, jnp.zeros((ROWS, LANES), jnp.float32))
    if with_extra:
        held, stage = refs[n + 2], refs[n + 3]
        area = pl.ds(local * count * ROWS, plan.more(local))
        pad = plan.held - plan.spare
        for g in range(n):
            stage[g] = vals[g][area, :].astype(jnp.float32)
            for m in range(local):
                at_m = pl.ds(m * plan.spare, plan.spare)
                held[g * local + m, pl.ds(0, plan.spare), :] = stage[g, at_m, :]
                if pad:
                    held[g * local + m, pl.ds(plan.spare, pad), :] = jnp.zeros((pad, LANES), jnp.float32)

        def last_block(i, total):
            rows = pl.ds(pl.multiple_of(i * ROWS, ROWS), ROWS)

            def load(g, m):
                return held[g * local + m, rows, :].astype(jnp.bfloat16)

            def store(g, m, value):
                held[g * local + m, rows, :] = value.astype(jnp.float32)

            t = t_ref[pl.ds(pl.multiple_of((count + i) * ROWS, ROWS), ROWS), :]
            return count_block(n, local, counts, step, load, t, store, total)

        total = lax.fori_loop(0, plan.held // ROWS, last_block, total)
        for g in range(n):
            for m in range(local):
                at_m = pl.ds(m * plan.spare, plan.spare)
                stage[g, at_m, :] = held[g * local + m, pl.ds(0, plan.spare), :]
            grads[g][area, :] = stage[g].astype(jnp.bfloat16)
    total = jnp.sum(total) * (w * scale)
    loss[...] = before[...] + total if has_before else jnp.full(loss.shape, total, jnp.float32)


def count_terms(plan, count, values, target, weight, before, scale, members, with_extra, last):
    n = len(values)
    local = members // n
    shape = flat(local, count, TILE) if last else values[0]
    scratch = [pltpu.VMEM((members, ROWS, LANES), jnp.bfloat16)]
    if with_extra:
        scratch.append(pltpu.VMEM((members, plan.held, LANES), jnp.float32))
        scratch.append(pltpu.VMEM((n, plan.more(local), LANES), jnp.float32))
    cells = target.shape[0] * LANES
    return pl.pallas_call(
        functools.partial(count_kernel, plan, count, local, scale, before is not None, with_extra),
        out_shape=[jax.ShapeDtypeStruct(shape.shape, jnp.bfloat16)] * n
        + [jax.ShapeDtypeStruct((TILE, LANES), jnp.float32)],
        in_specs=[pl.BlockSpec(memory_space=pltpu.SMEM)] + [VMEM] * (n + (1 if before is None else 2)),
        out_specs=[VMEM] * (n + 1),
        scratch_shapes=scratch,
        cost_estimate=pl.CostEstimate(
            flops=members * members * 3 * cells, bytes_accessed=4 * members * cells, transcendentals=0
        ),
        compiler_params=PARAMS,
        name="count",
    )(weight, target, *values, *([] if before is None else [before]))


def attach_kernel(n, part, *refs):
    value = part[...]
    high = value.astype(jnp.bfloat16).astype(jnp.float32)
    mid = (value - high).astype(jnp.bfloat16).astype(jnp.float32)
    row = lax.broadcasted_iota(jnp.int32, value.shape, 0)
    terms = jnp.where(row == 0, high, jnp.where(row == 1, mid, value - high - mid))
    block = jnp.where(row < 3, terms, 0.0).astype(jnp.bfloat16)
    for out in refs[n:]:
        out[pl.ds(out.shape[0] - TILE, TILE), :] = block


def attach(pieces, part):
    n = len(pieces)
    return pl.pallas_call(
        functools.partial(attach_kernel, n),
        out_shape=[jax.ShapeDtypeStruct(p.shape, p.dtype) for p in pieces],
        in_specs=[VMEM] * (n + 1),
        out_specs=[VMEM] * n,
        input_output_aliases={i + 1: i for i in range(n)},
        compiler_params=PARAMS,
        name="attach",
    )(part, *pieces)


def spread_extra(plan, extra, edge, low, fold, rows, lead):
    for r in range(plan.left_tiles):
        for c in range(plan.cols):
            for at, spot, length in plan.runs((r * plan.cols + c) * TILE, TILE):
                fold[pl.ds(at, length), :] = extra[lead + (pl.ds(spot, length), slice(None))]
            low[lead + (pl.ds(r * TILE, TILE), pl.ds(c * LANES, LANES))] = fold[:TILE].astype(jnp.bfloat16)
    for at, spot, length in plan.runs(plan.low_rows, plan.folded):
        fold[pl.ds(at, length), :] = extra[lead + (pl.ds(spot, length), slice(None))]
    value = fold[...]
    for i in range(plan.folds):
        one = pltpu.roll(value, LANES - i * plan.tail, 1) if i else value
        rows[pl.ds(i * plan.folded, plan.folded), :] = one[: plan.folded]
    edge[lead + (slice(None), slice(None))] = rows[...].astype(jnp.bfloat16)


def edge_kernel(plan, count, *refs):
    n = plan.groups
    ins, (out, low, extra, stage, fold, rows) = refs[1 : n + 1], refs[n + 1 :]
    me = lax.axis_index("mem")
    members = out.shape[0]
    area = pl.ds(members * count * ROWS, plan.more(members))
    fold[...] = jnp.zeros_like(fold)
    for b in range(n):
        at = pl.multiple_of(partner(me, b) * plan.held, ROWS)
        stage[b] = ins[b][area, :].astype(jnp.float32)
        for m in range(members):
            extra[m, pl.ds(at, plan.spare), :] = stage[b, pl.ds(m * plan.spare, plan.spare), :]
    for m in range(members):
        spread_extra(plan, extra, out, low, fold, rows, (m,))


def write_edge(plan, out, pieces, count):
    members = out.shape[0]
    n = plan.groups
    full = lambda s: pl.BlockSpec(s, lambda i, k=len(s): (0,) * k)
    low = (members, plan.left_tiles * TILE, plan.cols * LANES)
    return pl.pallas_call(
        functools.partial(edge_kernel, plan, count),
        grid=(1,),
        out_shape=[jax.ShapeDtypeStruct(out.shape, out.dtype), jax.ShapeDtypeStruct(low, out.dtype)],
        in_specs=[ANY] + [full(p.shape) for p in pieces],
        out_specs=[pl.BlockSpec((members, plan.channels, LANES), lambda i: (0, 0, plan.cols)), full(low)],
        scratch_shapes=[
            pltpu.VMEM((members, plan.held * n, LANES), jnp.float32),
            pltpu.VMEM((n, plan.more(members), LANES), jnp.float32),
            pltpu.VMEM((max(TILE, cdiv(plan.folded, TILE) * TILE), LANES), jnp.float32),
            pltpu.VMEM((plan.channels, LANES), jnp.float32),
        ],
        input_output_aliases={0: 0},
        compiler_params=PARAMS,
        name="write_edge",
    )(out, *pieces)


def put_kernel(plan, first, count, skip, last, with_low, *refs):
    n = plan.groups
    ins, refs = refs[skip : n + skip], refs[n + skip :]
    if last:
        part, out, loss, sem, held = refs
    elif with_low:
        low, out, sem = refs
    else:
        out, sem = refs
    me = lax.axis_index("mem")
    members = out.shape[0]
    copies = []
    for b in range(n):
        source = body_of(ins[b], members, count)
        for i in range(count):
            rows, cols = body_slices(plan, partner(me, b), first + i)
            copies.append(
                pltpu.make_async_copy(source.at[:, pl.ds(i * ROWS, ROWS), :], out.at[:, rows, cols], sem.at[len(copies)])
            )
    if with_low:
        rows, cols = pl.ds(plan.body_rows, low.shape[1]), pl.ds(0, low.shape[2])
        copies.append(pltpu.make_async_copy(low, out.at[:, rows, cols], sem.at[len(copies)]))
    for c in copies:
        c.start()
    if last:
        parts = [part[0:1, :]]
        for b in range(1, n):
            block = ins[b][pl.ds(members * count * ROWS, TILE), :].astype(jnp.float32)
            parts.append(block[0:1] + block[1:2] + block[2:3])
        while len(parts) > 1:
            parts = [x + y for x, y in zip(parts[::2], parts[1::2])]
        held[...] = parts[0]
        copies.append(pltpu.make_async_copy(held, loss, sem.at[len(copies)]))
        copies[-1].start()
    for c in copies:
        c.wait()


def put(plan, out, shape, pieces, first, count, low=None, part=None):
    n = plan.groups
    skip = 0 if out is None else 1
    last, with_low = part is not None, low is not None
    shapes = [jax.ShapeDtypeStruct(shape, jnp.bfloat16)]
    if last:
        shapes.append(jax.ShapeDtypeStruct((1, LANES), jnp.float32))
    more = ([part] if last else []) + ([low] if with_low else [])
    return pl.pallas_call(
        functools.partial(put_kernel, plan, first, count, skip, last, with_low),
        out_shape=shapes if last else shapes[0],
        in_specs=[ANY] * skip + [VMEM] * (n + len(more)),
        out_specs=[ANY, ANY] if last else ANY,
        scratch_shapes=[pltpu.SemaphoreType.DMA((n * count + len(more),))]
        + ([pltpu.VMEM((1, LANES), jnp.float32)] if last else []),
        input_output_aliases={0: 0} if skip else {},
        compiler_params=PARAMS,
        name="put",
    )(*([out] if skip else []), *pieces, *more)


def exchange(pieces, groups, order):
    out = list(pieces)
    for b in order:
        out[b] = lax.ppermute(pieces[b], "mem", pairs_of(b, groups))
    return out


def butterfly(value, axis, size):
    step = 1
    while step < size:
        value = value + lax.ppermute(value, axis, pairs_of(step, size))
        step *= 2
    return value


def split(total, parts):
    edges = [round(total * sum(parts[:i]) / sum(parts)) for i in range(len(parts) + 1)]
    return [b - a for a, b in zip(edges, edges[1:])]


PARTS = (3, 6, 4)
EXTRA_IN = 1


def orders(groups, count):
    near = [b for b in range(1, groups)]
    first = [groups - 1] + [b for b in range(1, groups - 1)]
    end = near[1:] + near[:1]
    return [first if k == 0 else near for k in range(count)], [near] * (count - 1) + [end]


def on_device(groups, lats, ensemble, truth, row_weight):
    local, channels, rows, cells = ensemble.shape
    members = local * groups
    plan = Plan(channels, cells, groups)
    ens = ensemble.reshape(local, channels, cells)
    tru = truth.reshape(channels, cells)
    scale = 1.0 / (members * (members - 1.0)) / (channels * rows * lats * cells)
    sizes = split(plan.body + plan.held // ROWS, PARTS)
    sizes[EXTRA_IN] -= plan.held // ROWS
    count = len(sizes)
    chunks = [(sum(sizes[:k]), sizes[k]) for k in range(count)]
    ins, outs = orders(groups, count)

    got = []
    for k in range(count):
        if k == EXTRA_IN:
            made = pack_rest(plan, ens, tru, chunks, k)
            pieces, target = made[:groups], made[groups:]
        else:
            every = tuple(range(groups))
            if k == 0:
                source = pltpu.with_memory_space_constraint(ens, pltpu.HBM)
                head = pack(plan, source, *chunks[k], every[-1:])
                pieces = list(pack(plan, ens, *chunks[k], every[:-1])) + list(head)
            else:
                pieces = pack(plan, ens, *chunks[k], every)
        got.append(exchange(pieces, groups, ins[k]))
    part, back = None, []
    for k in range(count):
        last = k == count - 1
        *grad, part = count_terms(
            plan, sizes[k], got[k], target[k], row_weight, part, scale, members, k == EXTRA_IN, last
        )
        if last:
            part = butterfly(part, "lat", lats)
            grad = grad[:1] + list(attach(grad[1:], part))
        back.append(exchange(grad, groups, outs[k]))
    out = None
    for k in range(count):
        low = None
        if k == EXTRA_IN:
            out, low = write_edge(plan, out, back[k], sizes[k])
        out = put(plan, out, ens.shape, back[k], *chunks[k], low, part if k == count - 1 else None)
    out, loss = out
    return loss[0, 0], out.reshape(ensemble.shape)


def solution(mesh):
    placed = (P("mem", None, "lat", None), P(None, "lat", None), P("lat"))
    groups = mesh.shape["mem"]
    return jax.shard_map(
        functools.partial(on_device, groups, mesh.shape["lat"]),
        mesh=mesh,
        in_specs=placed,
        out_specs=(P(), P("mem", None, "lat", None)),
        check_vma=False,
    )
```
